8 devices in a mesh: dp: 1 (over z), sp: 8 (over y, x, core).
Axes of the slice: x: 2, y: 2, z: 1, core: 2. Of those that a mesh axis runs over, the one named last changes fastest.
Arguments:
- x_in: bfloat16 [2, 8192, 384], P('dp', 'sp')
- grad_y: bfloat16 [2, 8192, 384], P('dp', 'sp')
- ln_gain: float32 [384], replicated
- ln_bias: float32 [384], replicated
- w_qkv: bfloat16 [384, 1152], replicated
- w_out: bfloat16 [384, 384], replicated
- temp_tau: float32 [8], replicated
Outputs:
- output 1: bfloat16 [2, 8192, 384], P('dp', 'sp')
- output 2: bfloat16 [2, 8192, 384], P('dp', 'sp')
- output 3: bfloat16 [384, 1152], P(('dp', 'sp'))
- output 4: bfloat16 [384, 384], P(('dp', 'sp'))
- output 5: float32 [384], P('dp')
- output 6: float32 [384], P('dp')
- output 7: float32 [8], P('dp')
All inputs are finite; a program needn't handle non-finite values.
Results may differ from the reference program's by a relative error of at most 0.00912741.
Values are sent between devices in bfloat16 or wider.
A program may use at most 1 GiB of HBM per device.

```python
import math
import jax
import jax.numpy as jnp
from jax import lax

NUM_IMAGES = 2
SEQ_LEN = 8192
MODEL_DIM = 384
NUM_HEADS = 8
HEAD_DIM = MODEL_DIM // NUM_HEADS
LN_EPS = 1e-6


def setup_inputs(seed: int = 0, part: int = 0) -> dict:
    base_key = jax.random.key(seed)
    part_keys = jax.random.split(jax.random.fold_in(base_key, part), 4)
    shared_keys = jax.random.split(base_key, 5)
    positions = (jnp.arange(SEQ_LEN, dtype=jnp.float32) + 0.5) / SEQ_LEN
    frequencies = jnp.arange(1, 5, dtype=jnp.float32)
    phases = 2.0 * math.pi * jax.random.uniform(part_keys[0], (NUM_IMAGES, 4), jnp.float32)
    wave_basis = jnp.sin(2.0 * math.pi * frequencies[None, :, None] * positions[None, None, :] + phases[:, :, None])
    mode_vecs = jax.random.normal(part_keys[1], (NUM_IMAGES, 4, MODEL_DIM), jnp.float32)
    trend_part = jnp.einsum("bmn,bmd->bnd", wave_basis, mode_vecs)
    noise_part = jax.random.normal(part_keys[2], (NUM_IMAGES, SEQ_LEN, MODEL_DIM), jnp.float32)
    x_in = (noise_part + trend_part).astype(jnp.bfloat16)
    grad_y = jax.random.normal(part_keys[3], (NUM_IMAGES, SEQ_LEN, MODEL_DIM), jnp.float32).astype(jnp.bfloat16)
    fan_scale = MODEL_DIM ** -0.5
    ln_gain = 1.0 + 0.3 * jax.random.normal(shared_keys[0], (MODEL_DIM,), jnp.float32)
    ln_bias = 0.3 * jax.random.normal(shared_keys[1], (MODEL_DIM,), jnp.float32)
    w_qkv = (fan_scale * jax.random.normal(shared_keys[2], (MODEL_DIM, 3 * MODEL_DIM), jnp.float32)).astype(jnp.bfloat16)
    w_out = (fan_scale * jax.random.normal(shared_keys[3], (MODEL_DIM, MODEL_DIM), jnp.float32)).astype(jnp.bfloat16)
    temp_tau = jax.random.uniform(shared_keys[4], (NUM_HEADS,), jnp.float32, 3.0, 6.0)
    return {"x_in": x_in, "grad_y": grad_y, "ln_gain": ln_gain, "ln_bias": ln_bias, "w_qkv": w_qkv, "w_out": w_out, "temp_tau": temp_tau}


def block_forward(x_in, ln_gain, ln_bias, w_qkv, w_out, temp_tau):
    x_f32 = x_in.astype(jnp.float32)
    mean_x = jnp.mean(x_f32, axis=-1, keepdims=True)
    centered = x_f32 - mean_x
    var_x = jnp.mean(centered * centered, axis=-1, keepdims=True)
    normed = (centered * lax.rsqrt(var_x + LN_EPS) * ln_gain + ln_bias).astype(jnp.bfloat16)
    qkv_all = jnp.dot(normed.reshape(NUM_IMAGES * SEQ_LEN, MODEL_DIM), w_qkv, preferred_element_type=jnp.float32).astype(jnp.bfloat16)
    qkv_heads = qkv_all.reshape(NUM_IMAGES, SEQ_LEN, 3, NUM_HEADS, HEAD_DIM)
    q_f32 = qkv_heads[:, :, 0].astype(jnp.float32)
    k_f32 = qkv_heads[:, :, 1].astype(jnp.float32)
    v_f32 = qkv_heads[:, :, 2].astype(jnp.float32)
    gram_state = jnp.einsum("bnhi,bnhj->bhij", q_f32, k_f32)
    sumsq_q = jnp.sum(q_f32 * q_f32, axis=1)
    sumsq_k = jnp.sum(k_f32 * k_f32, axis=1)
    logits = temp_tau[None, :, None, None] * gram_state / jnp.sqrt(sumsq_q[..., :, None] * sumsq_k[..., None, :])
    attn_bf16 = jax.nn.softmax(logits, axis=-1).astype(jnp.bfloat16)
    heads_out = jnp.einsum("bhij,bnhj->bnhi", attn_bf16.astype(jnp.float32), v_f32).astype(jnp.bfloat16)
    projected = jnp.dot(heads_out.reshape(NUM_IMAGES * SEQ_LEN, MODEL_DIM), w_out, preferred_element_type=jnp.float32)
    return (x_f32 + projected.reshape(NUM_IMAGES, SEQ_LEN, MODEL_DIM)).astype(jnp.bfloat16)


def reference(x_in, grad_y, ln_gain, ln_bias, w_qkv, w_out, temp_tau):
    y_out, pullback = jax.vjp(block_forward, x_in, ln_gain, ln_bias, w_qkv, w_out, temp_tau)
    grad_x, grad_gain, grad_bias, grad_wqkv, grad_wout, grad_tau = pullback(grad_y)
    return (y_out, grad_x, grad_wqkv, grad_wout, grad_gain, grad_bias, grad_tau)
```

```python
import functools

import jax
import jax.numpy as jnp
from jax import lax
from jax.experimental import pallas as pl
from jax.experimental.pallas import tpu as pltpu
from jax.sharding import PartitionSpec as P

LN_EPS = 1e-6
MESH = pl.DeviceIdType.MESH
F32 = jnp.float32
BF16 = jnp.bfloat16
LANES = 128
SLAB_ROWS = 56
BACK_ROWS = 64


def dot(a, b, ca, cb):
    return lax.dot_general(a, b, (((ca,), (cb,)), ((), ())), preferred_element_type=F32)


def body(images, tokens, dim, heads, n,
         x_hbm, dy_hbm, gain_ref, bias_ref, wqkv_hbm, wout_hbm, tau_ref,
         y_hbm, dx_hbm, gwqkv_ref, gwout_ref, ggain_ref, gbias_ref, gtau_ref,
         x_v, dy_v, wqkv_v, wout_v, xhat_v, rstd_v, u_v, qkv_v, do_v, o_v, dqkv_v, y_v, dx_v,
         slab_send, slab_recv, back, bd_a, bd_g, cq_v, ck_v,
         part, pair_recv, chip_sum, chip_recv, ln_all,
         load_sem, store_sem, slab_ssem, slab_rsem, back_ssem, back_rsem,
         pair_ssem, pair_rsem, chip_ssem, chip_rsem, ln_ssem, ln_rsem):
    hd = dim // heads
    tiles = dim // LANES
    me = lax.axis_index("sp")
    core = lax.rem(me, 2)
    chip = me // 2
    partner = me + 1 - 2 * core
    chip_x = chip + 1 - 2 * lax.rem(chip, 2)
    chip_y = lax.rem(chip + 2, 4)
    chip_d = lax.rem(chip_x + 2, 4)
    chips = (chip_x, chip_y, chip_d)

    def dev(d):
        return {"sp": d}

    def rows(b):
        return pl.ds(pl.multiple_of(b * tokens, tokens), tokens)

    def load_x(b):
        return pltpu.make_async_copy(x_hbm.at[b], x_v.at[rows(b)], load_sem.at[b])

    def load_dy(b):
        return pltpu.make_async_copy(dy_hbm.at[b], dy_v.at[rows(b)], load_sem.at[images + b])

    load_wqkv = pltpu.make_async_copy(wqkv_hbm, wqkv_v, load_sem.at[2 * images])
    load_wout = pltpu.make_async_copy(wout_hbm, wout_v, load_sem.at[2 * images + 1])
    load_x(0).start()
    load_wqkv.start()
    load_wout.start()
    load_dy(0).start()
    load_x(1).start()
    load_dy(1).start()

    barrier = pltpu.get_barrier_semaphore()
    for off in range(1, n):
        pl.semaphore_signal(barrier, inc=1, device_id=dev(lax.rem(me + off, n)), device_id_type=MESH)

    gain = gain_ref[...]
    bias = bias_ref[...]
    lane = lax.broadcasted_iota(jnp.int32, (hd, LANES), 1)
    row = lax.broadcasted_iota(jnp.int32, (hd, LANES), 0)
    lane1 = lax.broadcasted_iota(jnp.int32, (1, LANES), 1)

    def slab_copy(b, off):
        dst = lax.rem(me + off, n)
        return pltpu.make_async_remote_copy(
            src_ref=slab_send.at[b, dst], dst_ref=slab_recv.at[b, off - 1],
            send_sem=slab_ssem.at[b, off - 1], recv_sem=slab_rsem.at[b, off - 1],
            device_id=dev(dst), device_id_type=MESH)

    def back_copy(b, off):
        dst = lax.rem(me + off, n)
        return pltpu.make_async_remote_copy(
            src_ref=back.at[b, me], dst_ref=back.at[b, me],
            send_sem=back_ssem.at[b, off - 1], recv_sem=back_rsem.at[b, off - 1],
            device_id=dev(dst), device_id_type=MESH)

    def back_arrival(b, off):
        src = lax.rem(me + n - off, n)
        return pltpu.make_async_remote_copy(
            src_ref=back.at[b, src], dst_ref=back.at[b, src],
            send_sem=back_ssem.at[b, off - 1], recv_sem=back_rsem.at[b, off - 1],
            device_id=dev(lax.rem(me + off, n)), device_id_type=MESH)

    def phase1(b, carry):
        rs = rows(b)
        load_x(b).wait()

        @pl.when(b == 0)
        def _():
            load_wqkv.wait()

        xf = x_v[rs, :].astype(F32)
        mean = jnp.mean(xf, axis=-1, keepdims=True)
        cent = xf - mean
        rstd = lax.rsqrt(jnp.mean(cent * cent, axis=-1, keepdims=True) + LN_EPS)
        xhat = cent * rstd
        xhat_v[rs, :] = xhat
        rstd_v[rs, :] = rstd
        u = (xhat * gain + bias).astype(BF16)
        u_v[rs, :] = u
        qkv_v[rs, :] = dot(u, wqkv_v[...], 1, 0).astype(BF16)
        q = qkv_v[rs, 0:dim]
        k = qkv_v[rs, dim:2 * dim]
        v = qkv_v[rs, 2 * dim:3 * dim]
        gram = dot(q, k, 0, 0)
        qf = q.astype(F32)
        kf = k.astype(F32)
        ssq = jnp.sum(qf * qf, axis=0, keepdims=True)
        ssk = jnp.sum(kf * kf, axis=0, keepdims=True)

        @pl.when(b == 0)
        def _():
            load_wout.wait()

        load_dy(b).wait()
        do = dot(dy_v[rs, :], wout_v[...], 1, 1).astype(BF16)
        do_v[rs, :] = do
        dprob = dot(do, v, 0, 0)

        for h in range(heads):
            g_sum = None
            q_row = None
            for t in range(tiles):
                lo, hi = max(h * hd, t * LANES), min((h + 1) * hd, (t + 1) * LANES)
                if lo >= hi:
                    continue
                cols = slice(t * LANES, (t + 1) * LANES)
                mask = (lane >= lo - t * LANES) & (lane < hi - t * LANES)
                mask1 = mask[0:1, :]
                g_t = jnp.where(mask, gram[h * hd:(h + 1) * hd, cols], 0.0)
                p_t = jnp.where(mask, dprob[h * hd:(h + 1) * hd, cols], 0.0)
                q_t = jnp.where(mask1, ssq[:, cols], 0.0)
                k_t = jnp.where(mask1, ssk[:, cols], 0.0)
                if g_sum is None:
                    g_sum, p_sum, q_row, k_row = g_t, p_t, q_t, k_t
                else:
                    g_sum, p_sum, q_row, k_row = g_sum + g_t, p_sum + p_t, q_row + q_t, k_row + k_t
            s = (h * hd) % LANES
            to_low = (LANES - s) % LANES
            to_high = (LANES - s + 64) % LANES

            def roll(val, amount):
                return pltpu.roll(val, amount, 1) if amount else val

            slab_send[b, h, 0:hd, :] = roll(g_sum, to_low) + roll(p_sum, to_high)
            qk = jnp.concatenate([q_row, k_row, jnp.zeros((6, LANES), F32)], axis=0)
            slab_send[b, h, hd:SLAB_ROWS, :] = roll(qk, to_low)

        @pl.when(b == 0)
        def _():
            pl.semaphore_wait(barrier, n - 1)

        for off in range(1, n):
            slab_copy(b, off).start()
        return carry

    lax.fori_loop(0, images, phase1, 0)

    lane8 = lax.broadcasted_iota(jnp.int32, (1, LANES), 1)
    tau_row = tau_ref[...]
    tau = jnp.sum(jnp.where(lane8 == me, tau_row, 0.0), axis=1, keepdims=True)
    eye = lane == row
    live = lane < hd
    live1 = lane1 < hd

    def owner(b, tau_sum):
        for off in range(1, n):
            slab_copy(b, off).wait_recv()
        total = slab_send[b, me]
        for off in range(1, n):
            total = total + slab_recv[b, off - 1]
        gram = total[0:hd, :]
        dprob = pltpu.roll(gram, 64, 1).astype(BF16).astype(F32)
        ssq = total[hd:hd + 1, :]
        ssk = total[hd + 1:hd + 2, :]
        rq = lax.rsqrt(ssq)
        rk = lax.rsqrt(ssk)
        rq_col = jnp.sum(jnp.where(eye, rq, 0.0), axis=1, keepdims=True)
        scale = jnp.where(live, tau * rq_col * rk, 0.0)
        logits = jnp.where(live, gram * scale, 0.0)
        top = jnp.max(jnp.where(live, logits, -jnp.inf), axis=1, keepdims=True)
        e = jnp.where(live, jnp.exp(logits - top), 0.0)
        p = e / jnp.sum(e, axis=1, keepdims=True)
        dprob = jnp.where(live, dprob, 0.0)
        glog = p * (dprob - jnp.sum(p * dprob, axis=1, keepdims=True))
        weighted = glog * logits
        w_row = jnp.sum(weighted, axis=1, keepdims=True)
        tau_sum = tau_sum + jnp.sum(w_row, axis=0, keepdims=True)
        cq = -jnp.sum(jnp.where(eye, w_row, 0.0), axis=0, keepdims=True)
        cq = jnp.where(live1, cq / ssq, 0.0)
        ck = jnp.where(live1, -jnp.sum(weighted, axis=0, keepdims=True) / ssk, 0.0)
        dgram = glog * scale
        back[b, me, 0:hd, :] = (p + pltpu.roll(dgram, 64, 1)).astype(BF16)
        c_row = cq + pltpu.roll(ck, 64, 1)
        back[b, me, hd:BACK_ROWS, :] = jnp.broadcast_to(c_row, (BACK_ROWS - hd, LANES)).astype(BF16)
        for off in range(1, n):
            back_copy(b, off).start()
        return tau_sum

    tau_sum = jnp.zeros((1, 1), F32)
    for b in range(images):
        tau_sum = owner(b, tau_sum)

    for b in range(images):
        for off in range(1, n):
            back_arrival(b, off).wait_recv()
        cq = [jnp.zeros((1, LANES), F32) for _ in range(tiles)]
        ck = [jnp.zeros((1, LANES), F32) for _ in range(tiles)]
        for h in range(heads):
            got = back[b, h].astype(F32)
            s = (h * hd) % LANES
            low = pltpu.roll(got, s, 1) if s else got
            high = pltpu.roll(got, (s + 64) % LANES, 1) if (s + 64) % LANES else got
            a_tiles, g_tiles = [], []
            for t in range(tiles):
                lo, hi = max(h * hd, t * LANES), min((h + 1) * hd, (t + 1) * LANES)
                if lo >= hi:
                    a_tiles.append(jnp.zeros((hd, LANES), F32))
                    g_tiles.append(jnp.zeros((hd, LANES), F32))
                    continue
                mask = (lane >= lo - t * LANES) & (lane < hi - t * LANES)
                mask1 = mask[0:1, :]
                a_tiles.append(jnp.where(mask, low[0:hd, :], 0.0))
                g_tiles.append(jnp.where(mask, high[0:hd, :], 0.0))
                cq[t] = cq[t] + jnp.where(mask1, low[hd:hd + 1, :], 0.0)
                ck[t] = ck[t] + jnp.where(mask1, high[hd:hd + 1, :], 0.0)
            bd_a[b, h * hd:(h + 1) * hd, :] = jnp.concatenate(a_tiles, axis=1).astype(BF16)
            bd_g[b, h * hd:(h + 1) * hd, :] = jnp.concatenate(g_tiles, axis=1).astype(BF16)
        cq_v[b] = jnp.broadcast_to(jnp.concatenate(cq, axis=1), (8, dim))
        ck_v[b] = jnp.broadcast_to(jnp.concatenate(ck, axis=1), (8, dim))

    def pair_copy(c):
        return pltpu.make_async_remote_copy(
            src_ref=part.at[c, :, 1 - core], dst_ref=pair_recv.at[c],
            send_sem=pair_ssem.at[c], recv_sem=pair_rsem.at[c],
            device_id=dev(partner), device_id_type=MESH)

    def chip_copy(c, i):
        return pltpu.make_async_remote_copy(
            src_ref=chip_sum.at[c, chips[i]], dst_ref=chip_recv.at[c, i],
            send_sem=chip_ssem.at[c, i], recv_sem=chip_rsem.at[c, i],
            device_id=dev(chips[i] * 2 + core), device_id_type=MESH)

    def put_part(c, value):
        part[c] = value.reshape(4, 2, hd, dim)

    def rs_mid(c):
        pair_copy(c).wait_recv()
        chip_sum[c] = part[c, :, core] + pair_recv[c]
        for i in range(3):
            chip_copy(c, i).start()

    def rs_end(c):
        for i in range(3):
            chip_copy(c, i).wait_recv()
        total = chip_sum[c, chip]
        for i in range(3):
            total = total + chip_recv[c, i]
        return total.astype(BF16)

    def heads_out(b, carry):
        rs = rows(b)
        o_v[rs, :] = dot(qkv_v[rs, 2 * dim:3 * dim], bd_a[b], 1, 1).astype(BF16)
        return carry

    lax.fori_loop(0, images, heads_out, 0)
    put_part(0, dot(o_v[...], dy_v[...], 0, 0))
    pair_copy(0).start()

    def grad_v(b, carry):
        rs = rows(b)
        dqkv_v[rs, 2 * dim:3 * dim] = dot(do_v[rs, :], bd_a[b], 1, 0).astype(BF16)
        return carry

    lax.fori_loop(0, images, grad_v, 0)
    rs_mid(0)
    put_part(1, dot(u_v[...], dqkv_v[:, 2 * dim:3 * dim], 0, 0))
    pair_copy(1).start()

    def grad_q(b, carry):
        rs = rows(b)
        q = qkv_v[rs, 0:dim]
        k = qkv_v[rs, dim:2 * dim]
        dqkv_v[rs, 0:dim] = (dot(k, bd_g[b], 1, 1) + cq_v[b, 0:1, :] * q.astype(F32)).astype(BF16)
        return carry

    lax.fori_loop(0, images, grad_q, 0)
    rs_mid(1)
    put_part(2, dot(u_v[...], dqkv_v[:, 0:dim], 0, 0))
    pair_copy(2).start()

    def grad_k(b, carry):
        rs = rows(b)
        q = qkv_v[rs, 0:dim]
        k = qkv_v[rs, dim:2 * dim]
        dqkv_v[rs, dim:2 * dim] = (dot(q, bd_g[b], 1, 0) + ck_v[b, 0:1, :] * k.astype(F32)).astype(BF16)
        return carry

    lax.fori_loop(0, images, grad_k, 0)
    rs_mid(2)
    put_part(3, dot(u_v[...], dqkv_v[:, dim:2 * dim], 0, 0))
    pair_copy(3).start()

    def store_y(b):
        return pltpu.make_async_copy(y_v.at[rows(b)], y_hbm.at[b], store_sem.at[b])

    def store_dx(b):
        return pltpu.make_async_copy(dx_v.at[rows(b)], dx_hbm.at[b], store_sem.at[images + b])

    def out_y(b, carry):
        rs = rows(b)
        y_v[rs, :] = (x_v[rs, :].astype(F32) + dot(o_v[rs, :], wout_v[...], 1, 0)).astype(BF16)
        store_y(b).start()
        return carry

    lax.fori_loop(0, images, out_y, 0)
    rs_mid(3)

    def out_dx(b, carry):
        sg, sb = carry
        rs = rows(b)
        du = dot(dqkv_v[rs, :], wqkv_v[...], 1, 1).astype(BF16).astype(F32)
        xhat = xhat_v[rs, :]
        sg = sg + jnp.sum(du * xhat, axis=0, keepdims=True)
        sb = sb + jnp.sum(du, axis=0, keepdims=True)
        a = du * gain
        ma = jnp.mean(a, axis=-1, keepdims=True)
        mx = jnp.mean(a * xhat, axis=-1, keepdims=True)
        dx_v[rs, :] = (dy_v[rs, :].astype(F32) + rstd_v[rs, :] * (a - ma - xhat * mx)).astype(BF16)
        store_dx(b).start()
        return sg, sb

    zero = jnp.zeros((1, dim), F32)
    sg, sb = lax.fori_loop(0, images, out_dx, (zero, zero))

    lane_d = lax.broadcasted_iota(jnp.int32, (1, dim), 1)
    st = jnp.where(lane_d == me, tau_sum / tau, 0.0)
    ln_all[me] = jnp.concatenate([sg, sb, st, jnp.zeros((5, dim), F32)], axis=0)

    def ln_copy(off):
        return pltpu.make_async_remote_copy(
            src_ref=ln_all.at[me], dst_ref=ln_all.at[me],
            send_sem=ln_ssem.at[off - 1], recv_sem=ln_rsem.at[off - 1],
            device_id=dev(lax.rem(me + off, n)), device_id_type=MESH)

    def ln_arrival(off):
        src = lax.rem(me + n - off, n)
        return pltpu.make_async_remote_copy(
            src_ref=ln_all.at[src], dst_ref=ln_all.at[src],
            send_sem=ln_ssem.at[off - 1], recv_sem=ln_rsem.at[off - 1],
            device_id=dev(lax.rem(me + off, n)), device_id_type=MESH)

    for off in range(1, n):
        ln_copy(off).start()

    gwout_ref[...] = rs_end(0)
    gwqkv_ref[:, 2 * dim:3 * dim] = rs_end(1)
    gwqkv_ref[:, 0:dim] = rs_end(2)
    for off in range(1, n):
        ln_arrival(off).wait_recv()
    sums = ln_all[0]
    for d in range(1, n):
        sums = sums + ln_all[d]
    ggain_ref[...] = sums[0:1, :]
    gbias_ref[...] = sums[1:2, :]
    gtau_ref[...] = sums[2:3, 0:LANES]
    gwqkv_ref[:, dim:2 * dim] = rs_end(3)

    for b in range(images):
        store_y(b).wait()
        store_dx(b).wait()
        for off in range(1, n):
            slab_copy(b, off).wait_send()
            back_copy(b, off).wait_send()
    for c in range(4):
        pair_copy(c).wait_send()
        for i in range(3):
            chip_copy(c, i).wait_send()
    for off in range(1, n):
        ln_copy(off).wait_send()


def solution(mesh):
    n = mesh.shape["sp"]

    def local_step(x_in, grad_y, ln_gain, ln_bias, w_qkv, w_out, temp_tau):
        images, tokens, dim = x_in.shape
        heads = temp_tau.shape[0]
        hd = dim // heads
        num = images * tokens
        any_spec = pl.BlockSpec(memory_space=pl.ANY)
        vmem = pl.BlockSpec(memory_space=pltpu.VMEM)
        dma = pltpu.SemaphoreType.DMA
        tau_row = jnp.pad(temp_tau[None, :], ((0, 0), (0, LANES - heads)))
        outs = pl.pallas_call(
            functools.partial(body, images, tokens, dim, heads, n),
            out_shape=(
                jax.ShapeDtypeStruct(x_in.shape, BF16),
                jax.ShapeDtypeStruct(x_in.shape, BF16),
                jax.ShapeDtypeStruct((hd, 3 * dim), BF16),
                jax.ShapeDtypeStruct((hd, dim), BF16),
                jax.ShapeDtypeStruct((1, dim), F32),
                jax.ShapeDtypeStruct((1, dim), F32),
                jax.ShapeDtypeStruct((1, LANES), F32),
            ),
            in_specs=[any_spec, any_spec, vmem, vmem, any_spec, any_spec, vmem],
            out_specs=(any_spec, any_spec, vmem, vmem, vmem, vmem, vmem),
            scratch_shapes=[
                pltpu.VMEM((num, dim), BF16),
                pltpu.VMEM((num, dim), BF16),
                pltpu.VMEM((dim, 3 * dim), BF16),
                pltpu.VMEM((dim, dim), BF16),
                pltpu.VMEM((num, dim), F32),
                pltpu.VMEM((num, 1), F32),
                pltpu.VMEM((num, dim), BF16),
                pltpu.VMEM((num, 3 * dim), BF16),
                pltpu.VMEM((num, dim), BF16),
                pltpu.VMEM((num, dim), BF16),
                pltpu.VMEM((num, 3 * dim), BF16),
                pltpu.VMEM((num, dim), BF16),
                pltpu.VMEM((num, dim), BF16),
                pltpu.VMEM((images, heads, SLAB_ROWS, LANES), F32),
                pltpu.VMEM((images, n - 1, SLAB_ROWS, LANES), F32),
                pltpu.VMEM((images, heads, BACK_ROWS, LANES), BF16),
                pltpu.VMEM((images, dim, dim), BF16),
                pltpu.VMEM((images, dim, dim), BF16),
                pltpu.VMEM((images, 8, dim), F32),
                pltpu.VMEM((images, 8, dim), F32),
                pltpu.VMEM((4, 4, 2, hd, dim), F32),
                pltpu.VMEM((4, 4, hd, dim), F32),
                pltpu.VMEM((4, 4, hd, dim), F32),
                pltpu.VMEM((4, 3, hd, dim), F32),
                pltpu.VMEM((n, 8, dim), F32),
                dma((2 * images + 2,)),
                dma((2 * images,)),
                dma((images, n - 1)), dma((images, n - 1)),
                dma((images, n - 1)), dma((images, n - 1)),
                dma((4,)), dma((4,)),
                dma((4, 3)), dma((4, 3)),
                dma((n - 1,)), dma((n - 1,)),
            ],
            compiler_params=pltpu.CompilerParams(collective_id=0, has_side_effects=True, vmem_limit_bytes=56 * 2**20),
            name="xca_step",
        )(x_in, grad_y, ln_gain[None, :], ln_bias[None, :], w_qkv, w_out, tau_row)
        y, dx, gwqkv, gwout, ggain, gbias, gtau = outs
        return y, dx, gwqkv, gwout, ggain[0], gbias[0], gtau[0, :heads]

    token_spec = P("dp", "sp", None)
    return jax.shard_map(local_step, mesh=mesh, in_specs=(token_spec, token_spec, P(), P(), P(), P(), P()), out_specs=(token_spec, token_spec, P(("dp", "sp"), None), P(("dp", "sp"), None), P("dp"), P("dp"), P("dp")), check_vma=False)
```

```python
import functools

import jax
import jax.numpy as jnp
from jax import lax
from jax.experimental import pallas as pl
from jax.experimental.pallas import tpu as pltpu
from jax.sharding import PartitionSpec as P

LN_EPS = 1e-6
MESH = pl.DeviceIdType.MESH
KERNEL_VMEM = 63713280
F32 = jnp.float32
BF16 = jnp.bfloat16
LANES = 128
G_ROWS = 32
P_ROWS = 24
BACK_ROWS = 32
SPLIT = 3


def dot(a, b, ca, cb):
    return lax.dot_general(a, b, (((ca,), (cb,)), ((), ())), preferred_element_type=F32)


def roll(val, amount):
    amount = amount % LANES
    return pltpu.roll(val, amount, 1) if amount else val


def scope(name):
    return jax.named_scope(name)


def body(images, tokens, dim, heads, n,
         x_hbm, dy_hbm, gain_hbm, bias_hbm, wqkv_hbm, wout_hbm, tau_hbm,
         y_v, dx_v, gwqkv_ref, gwout_ref, sums_ref,
         x_v, dy_v, gain_v, bias_v, tau_v, wqkv_v, wout_v, xhat_v, rstd_v, du_v, u_v, qkv_v, do_v, o_v, dqkv_v,
         g_send, g_recv, p_send, p_recv, back_a, back_g, bd_a, bd_g, cq_v, ck_v,
         part, pair_recv, chip_sum, x_recv, y_recv, x_send2, y_send2, x_recv2, y_recv2, ln_all,
         load_sem, g_ssem, g_rsem, p_ssem, p_rsem, a_ssem, a_rsem, d_ssem, d_rsem,
         pair_ssem, pair_rsem, st_ssem, st_rsem, ln_ssem, ln_rsem):
    hd = dim // heads
    half = hd // 2
    tiles = dim // LANES
    me = lax.axis_index("sp")
    core = lax.rem(me, 2)
    chip = me // 2
    px = lax.rem(chip, 2)
    py = chip // 2
    partner = me + 1 - 2 * core
    dev_x = me + 2 - 4 * px
    dev_y = me + 4 - 8 * py

    def dev(d):
        return {"sp": d}

    def rows(b):
        return pl.ds(pl.multiple_of(b * tokens, tokens), tokens)

    def load_x(b):
        return pltpu.make_async_copy(x_hbm.at[b], x_v.at[rows(b)], load_sem.at[b])

    def load_dy(b):
        return pltpu.make_async_copy(dy_hbm.at[b], dy_v.at[rows(b)], load_sem.at[images + b])

    load_wqkv = pltpu.make_async_copy(wqkv_hbm, wqkv_v, load_sem.at[2 * images])
    load_wout = pltpu.make_async_copy(wout_hbm, wout_v, load_sem.at[2 * images + 1])
    load_gain = pltpu.make_async_copy(gain_hbm, gain_v, load_sem.at[2 * images + 2])
    load_bias = pltpu.make_async_copy(bias_hbm, bias_v, load_sem.at[2 * images + 3])
    load_tau = pltpu.make_async_copy(tau_hbm, tau_v, load_sem.at[2 * images + 4])
    load_x(0).start()
    load_gain.start()
    load_bias.start()
    load_wqkv.start()
    load_x(1).start()
    load_wout.start()
    load_dy(0).start()
    load_dy(1).start()
    load_tau.start()

    barrier = pltpu.get_barrier_semaphore()
    for off in range(1, n):
        pl.semaphore_signal(barrier, inc=1, device_id=dev(lax.rem(me + off, n)), device_id_type=MESH)

    lane = lax.broadcasted_iota(jnp.int32, (hd, LANES), 1)
    row = lax.broadcasted_iota(jnp.int32, (hd, LANES), 0)

    def pieces(h):
        base = 0 if h < SPLIT else LANES
        first = h * hd - base
        found = []
        for t in range(2):
            lo, hi = max(first, t * LANES), min(first + hd, (t + 1) * LANES)
            if lo < hi:
                found.append((t, lo - t * LANES, hi - t * LANES))
        return (0 if h < SPLIT else 1), first, found

    def head_block(blocks, h):
        which, first, found = pieces(h)
        total = None
        for t, lo, hi in found:
            tile = blocks[which][first:first + hd, t * LANES:(t + 1) * LANES]
            tile = jnp.where((lane >= lo) & (lane < hi), tile, 0.0)
            total = tile if total is None else total + tile
        return total

    def head_row(vec, h):
        total = None
        for t in range(tiles):
            lo, hi = max(h * hd, t * LANES), min((h + 1) * hd, (t + 1) * LANES)
            if lo < hi:
                mask = (lane[0:1, :] >= lo - t * LANES) & (lane[0:1, :] < hi - t * LANES)
                tile = jnp.where(mask, vec[:, t * LANES:(t + 1) * LANES], 0.0)
                total = tile if total is None else total + tile
        return total

    def pack(val, s):
        return roll(val[0:half, :], -s) + roll(val[half:hd, :], 64 - s)

    def unpack(val):
        return jnp.concatenate([val, roll(val, 64)], axis=0)

    def exchange(send, recv, ssem, rsem, b, off):
        dst = lax.rem(me + off, n)
        return pltpu.make_async_remote_copy(
            src_ref=send.at[b, dst], dst_ref=recv.at[b, off - 1],
            send_sem=ssem.at[b, off - 1], recv_sem=rsem.at[b, off - 1],
            device_id=dev(dst), device_id_type=MESH)

    def g_copy(b, off):
        return exchange(g_send, g_recv, g_ssem, g_rsem, b, off)

    def p_copy(b, off):
        return exchange(p_send, p_recv, p_ssem, p_rsem, b, off)

    def spread(buf, ssem, rsem, b, off, src):
        return pltpu.make_async_remote_copy(
            src_ref=buf.at[b, src], dst_ref=buf.at[b, src],
            send_sem=ssem.at[b, off - 1], recv_sem=rsem.at[b, off - 1],
            device_id=dev(lax.rem(me + off, n)), device_id_type=MESH)

    def a_copy(b, off):
        return spread(back_a, a_ssem, a_rsem, b, off, me)

    def a_arrival(b, off):
        return spread(back_a, a_ssem, a_rsem, b, off, lax.rem(me + n - off, n))

    def d_copy(b, off):
        return spread(back_g, d_ssem, d_rsem, b, off, me)

    def d_arrival(b, off):
        return spread(back_g, d_ssem, d_rsem, b, off, lax.rem(me + n - off, n))

    def phase_g(b, carry):
        rs = rows(b)
        load_x(b).wait()

        @pl.when(b == 0)
        def _():
            load_gain.wait()
            load_bias.wait()
            load_wqkv.wait()

        gain = gain_v[...].reshape(1, dim)
        bias = bias_v[...].reshape(1, dim)
        xf = x_v[rs, :].astype(F32)
        mean = jnp.mean(xf, axis=-1, keepdims=True)
        cent = xf - mean
        rstd = lax.rsqrt(jnp.mean(cent * cent, axis=-1, keepdims=True) + LN_EPS)
        xhat = cent * rstd
        xhat_v[rs, :] = xhat
        rstd_v[rs, :] = rstd
        u = (xhat * gain + bias).astype(BF16)
        u_v[rs, :] = u
        qkv_v[rs, :] = dot(u, wqkv_v[...], 1, 0).astype(BF16)
        q = qkv_v[rs, 0:dim]
        k = qkv_v[rs, dim:2 * dim]
        gram = (dot(q[:, 0:256], k[:, 0:256], 0, 0), dot(q[:, 128:384], k[:, 128:384], 0, 0))
        qf = q.astype(F32)
        kf = k.astype(F32)
        ssq = jnp.sum(qf * qf, axis=0, keepdims=True)
        ssk = jnp.sum(kf * kf, axis=0, keepdims=True)
        for h in range(heads):
            s = (h * hd) % LANES
            g_send[b, h, 0:half, :] = pack(head_block(gram, h), s)
            qk = jnp.concatenate([head_row(ssq, h), head_row(ssk, h), jnp.zeros((6, LANES), F32)], axis=0)
            g_send[b, h, half:G_ROWS, :] = roll(qk, -s)

        @pl.when(b == 0)
        def _():
            pl.semaphore_wait(barrier, n - 1)

        for off in range(1, n):
            g_copy(b, off).start()
        return carry

    def phase_p(b, carry):
        rs = rows(b)

        @pl.when(b == 0)
        def _():
            load_wout.wait()

        load_dy(b).wait()
        do = dot(dy_v[rs, :], wout_v[...], 1, 1).astype(BF16)
        do_v[rs, :] = do
        v = qkv_v[rs, 2 * dim:3 * dim]
        dprob = (dot(do[:, 0:256], v[:, 0:256], 0, 0), dot(do[:, 128:384], v[:, 128:384], 0, 0))
        for h in range(heads):
            p_send[b, h] = pack(head_block(dprob, h), (h * hd) % LANES)
        for off in range(1, n):
            p_copy(b, off).start()
        return carry

    with scope("phase_g"):
        lax.fori_loop(0, images, phase_g, 0)
    with scope("phase_p"):
        lax.fori_loop(0, images, phase_p, 0)

    load_tau.wait()
    tau = tau_v[me]
    eye = lane == row
    live = lane < hd
    live1 = live[0:1, :]

    def owner_a(b):
        with scope("wait_g"):
            for off in range(1, n):
                g_copy(b, off).wait_recv()
        total = g_send[b, me]
        for off in range(1, n):
            total = total + g_recv[b, off - 1]
        gram = unpack(total[0:half, :])
        ssq = total[half:half + 1, :]
        ssk = total[half + 1:half + 2, :]
        rq_col = jnp.sum(jnp.where(eye, lax.rsqrt(ssq), 0.0), axis=1, keepdims=True)
        scale = jnp.where(live, tau * rq_col * lax.rsqrt(ssk), 0.0)
        logits = jnp.where(live, gram * scale, 0.0)
        top = jnp.max(jnp.where(live, logits, -jnp.inf), axis=1, keepdims=True)
        e = jnp.where(live, jnp.exp(logits - top), 0.0)
        p = e / jnp.sum(e, axis=1, keepdims=True)
        back_a[b, me] = jnp.concatenate([pack(p, 0), jnp.zeros((BACK_ROWS - half, LANES), F32)], axis=0).astype(BF16)
        for off in range(1, n):
            a_copy(b, off).start()
        return p, logits, scale, ssq, ssk

    def owner_g(b, state):
        p, logits, scale, ssq, ssk = state
        with scope("wait_p"):
            for off in range(1, n):
                p_copy(b, off).wait_recv()
        total = p_send[b, me]
        for off in range(1, n):
            total = total + p_recv[b, off - 1]
        dprob = jnp.where(live, unpack(total), 0.0).astype(BF16).astype(F32)
        glog = p * (dprob - jnp.sum(p * dprob, axis=1, keepdims=True))
        weighted = glog * logits
        w_row = jnp.sum(weighted, axis=1, keepdims=True)
        cq = -jnp.sum(jnp.where(eye, w_row, 0.0), axis=0, keepdims=True)
        cq = jnp.where(live1, cq / ssq, 0.0)
        ck = jnp.where(live1, -jnp.sum(weighted, axis=0, keepdims=True) / ssk, 0.0)
        c_row = jnp.broadcast_to(cq + roll(ck, 64), (BACK_ROWS - half, LANES))
        back_g[b, me] = jnp.concatenate([pack(glog * scale, 0), c_row], axis=0).astype(BF16)
        for off in range(1, n):
            d_copy(b, off).start()
        return jnp.sum(w_row, axis=0, keepdims=True)

    def build(b, got_of, arrival, bd, name):
        with scope(name):
            for off in range(1, n):
                arrival(b, off).wait_recv()
        tails = []
        for h in range(heads):
            got = got_of[b, h].astype(F32)
            which, first, found = pieces(h)
            s = first % LANES
            low = roll(got[0:half, :], s)
            high = roll(got[0:half, :], s + 64)
            val = jnp.concatenate([low, high], axis=0)
            cols = [jnp.zeros((hd, LANES), F32) for _ in range(2)]
            for t, lo, hi in found:
                cols[t] = jnp.where((lane >= lo) & (lane < hi), val, 0.0)
            bd[b, which, first:first + hd, :] = jnp.concatenate(cols, axis=1).astype(BF16)
            tails.append(got[half:half + 1, :])
        return tails

    def clear(bd):
        for b in range(images):
            bd[b, 0, SPLIT * hd:256, :] = jnp.zeros((256 - SPLIT * hd, 256), BF16)
            bd[b, 1, 0:SPLIT * hd - LANES, :] = jnp.zeros((SPLIT * hd - LANES, 256), BF16)

    def build_a(b):
        build(b, back_a, a_arrival, bd_a, "wait_a")

    def build_g(b):
        tails = build(b, back_g, d_arrival, bd_g, "wait_d")
        for dst, shift in ((cq_v, 0), (ck_v, 64)):
            vec = [jnp.zeros((1, LANES), F32) for _ in range(tiles)]
            for h in range(heads):
                val = roll(tails[h], shift + h * hd)
                for t in range(tiles):
                    lo, hi = max(h * hd, t * LANES), min((h + 1) * hd, (t + 1) * LANES)
                    if lo < hi:
                        mask = (lane[0:1, :] >= lo - t * LANES) & (lane[0:1, :] < hi - t * LANES)
                        vec[t] = vec[t] + jnp.where(mask, val, 0.0)
            dst[b] = jnp.broadcast_to(jnp.concatenate(vec, axis=1), (8, dim))

    def per_head(tok, mats, transposed):
        c = 1 if transposed else 0
        left = dot(tok[:, 0:256], mats[0], 1, c)
        right = dot(tok[:, 128:384], mats[1], 1, c)
        return jnp.concatenate([left[:, 0:128], left[:, 128:256] + right[:, 0:128], right[:, 128:256]], axis=1)

    def pair_copy(c):
        return pltpu.make_async_remote_copy(
            src_ref=part.at[c, :, :, 1 - core], dst_ref=pair_recv.at[c],
            send_sem=pair_ssem.at[c], recv_sem=pair_rsem.at[c],
            device_id=dev(partner), device_id_type=MESH)

    def stage_copies(c, stage):
        if stage == 0:
            refs = ((chip_sum.at[c, :, 1 - px, 0], x_recv.at[c], dev_x),
                    (chip_sum.at[c, 1 - py, :, 1], y_recv.at[c], dev_y))
        else:
            refs = ((x_send2.at[c], x_recv2.at[c], dev_x), (y_send2.at[c], y_recv2.at[c], dev_y))
        return [pltpu.make_async_remote_copy(
            src_ref=src, dst_ref=dst, send_sem=st_ssem.at[c, stage, i], recv_sem=st_rsem.at[c, stage, i],
            device_id=dev(d), device_id_type=MESH) for i, (src, dst, d) in enumerate(refs)]

    def rs0(c, value):
        part[c] = value.reshape(2, 2, 2, 2, half, dim)
        pair_copy(c).start()

    def rs1(c):
        with scope("wait_pair"):
            pair_copy(c).wait_recv()
        chip_sum[c] = part[c, :, :, core] + pair_recv[c]
        for copy in stage_copies(c, 0):
            copy.start()

    def rs2(c):
        with scope("wait_st0"):
            for copy in stage_copies(c, 0):
                copy.wait_recv()
        x_send2[c] = chip_sum[c, py, 1 - px, 1] + y_recv[c, 1 - px]
        y_send2[c] = chip_sum[c, 1 - py, px, 0] + x_recv[c, 1 - py]
        for copy in stage_copies(c, 1):
            copy.start()

    def rs3(c):
        own_a = chip_sum[c, py, px, 0] + x_recv[c, py]
        own_b = chip_sum[c, py, px, 1] + y_recv[c, px]
        with scope("wait_st1"):
            for copy in stage_copies(c, 1):
                copy.wait_recv()
        return jnp.concatenate([own_a + y_recv2[c], own_b + x_recv2[c]], axis=0).astype(BF16)

    def heads_out(b):
        rs = rows(b)
        o_v[rs, :] = per_head(qkv_v[rs, 2 * dim:3 * dim], bd_a[b], True).astype(BF16)

    def grad_v(b):
        rs = rows(b)
        dqkv_v[rs, 2 * dim:3 * dim] = per_head(do_v[rs, :], bd_a[b], False).astype(BF16)

    def grad_q(b):
        rs = rows(b)
        q = qkv_v[rs, 0:dim]
        k = qkv_v[rs, dim:2 * dim]
        dqkv_v[rs, 0:dim] = (per_head(k, bd_g[b], True) + cq_v[b, 0:1, :] * q.astype(F32)).astype(BF16)

    def grad_k(b):
        rs = rows(b)
        q = qkv_v[rs, 0:dim]
        k = qkv_v[rs, dim:2 * dim]
        dqkv_v[rs, dim:2 * dim] = (per_head(q, bd_g[b], False) + ck_v[b, 0:1, :] * k.astype(F32)).astype(BF16)

    def out_y(b):
        rs = rows(b)
        y_v[rs, :] = (x_v[rs, :].astype(F32) + dot(o_v[rs, :], wout_v[...], 1, 0)).astype(BF16)

    def grad_u(b):
        rs = rows(b)
        du = dot(dqkv_v[rs, :], wqkv_v[...], 1, 1).astype(BF16)
        du_v[rs, :] = du
        du = du.astype(F32)
        return jnp.sum(du * xhat_v[rs, :], axis=0, keepdims=True), jnp.sum(du, axis=0, keepdims=True)

    def out_dx(b):
        rs = rows(b)
        gain = gain_v[...].reshape(1, dim)
        xhat = xhat_v[rs, :]
        a = du_v[rs, :].astype(F32) * gain
        ma = jnp.mean(a, axis=-1, keepdims=True)
        mx = jnp.mean(a * xhat, axis=-1, keepdims=True)
        dx_v[rs, :] = (dy_v[rs, :].astype(F32) + rstd_v[rs, :] * (a - ma - xhat * mx)).astype(BF16)

    clear(bd_a)
    clear(bd_g)
    with scope("owner_a0"):
        state0 = owner_a(0)
    with scope("owner_a1"):
        state1 = owner_a(1)
    with scope("owner_g0"):
        w0 = owner_g(0, state0)
    build_a(0)
    with scope("heads_out"):
        heads_out(0)
    with scope("grad_v"):
        grad_v(0)
    with scope("owner_g1"):
        w1 = owner_g(1, state1)
    build_a(1)
    with scope("heads_out"):
        heads_out(1)
    with scope("part0"):
        rs0(0, dot(o_v[...], dy_v[...], 0, 0))
    with scope("grad_v"):
        grad_v(1)
    with scope("part1"):
        rs0(1, dot(u_v[...], dqkv_v[:, 2 * dim:3 * dim], 0, 0))
    rs1(0)
    build_g(0)
    with scope("grad_q"):
        grad_q(0)
    build_g(1)
    with scope("grad_q"):
        grad_q(1)
    rs1(1)
    with scope("part2"):
        rs0(2, dot(u_v[...], dqkv_v[:, 0:dim], 0, 0))
    with scope("grad_k"):
        grad_k(0)
    with scope("grad_k"):
        grad_k(1)
    rs1(2)
    with scope("part3"):
        rs0(3, dot(u_v[...], dqkv_v[:, dim:2 * dim], 0, 0))
    rs2(0)
    with scope("grad_u"):
        sg0, sb0 = grad_u(0)
    rs1(3)
    rs2(1)
    with scope("grad_u"):
        sg1, sb1 = grad_u(1)

    sg = sg0 + sg1
    sb = sb0 + sb1
    st = jnp.where(lane[0:1, :] == me, (w0 + w1) / tau, 0.0)
    ln_rows = [val[:, t * LANES:(t + 1) * LANES] for val in (sg, sb) for t in range(tiles)]
    ln_all[me] = jnp.concatenate(ln_rows + [st, jnp.zeros((1, LANES), F32)], axis=0)

    def ln_copy(off, src):
        return pltpu.make_async_remote_copy(
            src_ref=ln_all.at[src], dst_ref=ln_all.at[src],
            send_sem=ln_ssem.at[off - 1], recv_sem=ln_rsem.at[off - 1],
            device_id=dev(lax.rem(me + off, n)), device_id_type=MESH)

    for off in range(1, n):
        ln_copy(off, me).start()

    rs2(2)
    with scope("out_dx"):
        out_dx(0)
    with scope("out_y"):
        out_y(0)
    rs2(3)
    with scope("out_dx"):
        out_dx(1)
    with scope("out_y"):
        out_y(1)
    gwout_ref[...] = rs3(0)
    gwqkv_ref[:, 2 * dim:3 * dim] = rs3(1)
    gwqkv_ref[:, 0:dim] = rs3(2)
    gwqkv_ref[:, dim:2 * dim] = rs3(3)
    with scope("wait_ln"):
        for off in range(1, n):
            ln_copy(off, lax.rem(me + n - off, n)).wait_recv()
    sums = ln_all[0]
    for d in range(1, n):
        sums = sums + ln_all[d]
    sums_ref[...] = sums

    with scope("final"):
        for b in range(images):
            for off in range(1, n):
                g_copy(b, off).wait_send()
                p_copy(b, off).wait_send()
                a_copy(b, off).wait_send()
                d_copy(b, off).wait_send()
        for c in range(4):
            pair_copy(c).wait_send()
            for stage in range(2):
                for copy in stage_copies(c, stage):
                    copy.wait_send()
        for off in range(1, n):
            ln_copy(off, me).wait_send()


def finish(dim, heads, y_v, dx_v, gwqkv_v, gwout_v, sums_v,
           y_hbm, dx_hbm, gwqkv_hbm, gwout_hbm, ggain_ref, gbias_ref, gtau_ref, sem):
    pairs = ((y_v, y_hbm), (dx_v, dx_hbm), (gwqkv_v, gwqkv_hbm), (gwout_v, gwout_hbm))
    copies = [pltpu.make_async_copy(src, dst, sem.at[i]) for i, (src, dst) in enumerate(pairs)]
    for copy in copies:
        copy.start()
    tiles = dim // LANES
    for t in range(tiles):
        ggain_ref[t * LANES:(t + 1) * LANES] = sums_v[t, :]
        gbias_ref[t * LANES:(t + 1) * LANES] = sums_v[tiles + t, :]
    gtau_ref[...] = sums_v[2 * tiles, 0:heads]
    for copy in copies:
        copy.wait()


def solution(mesh):
    n = mesh.shape["sp"]

    def local_step(x_in, grad_y, ln_gain, ln_bias, w_qkv, w_out, temp_tau):
        images, tokens, dim = x_in.shape
        heads = temp_tau.shape[0]
        hd = dim // heads
        half = hd // 2
        num = images * tokens
        hbm = pl.BlockSpec(memory_space=pltpu.HBM)
        vmem = pl.BlockSpec(memory_space=pltpu.VMEM)
        dma = pltpu.SemaphoreType.DMA
        params = pltpu.CompilerParams(collective_id=0, has_side_effects=True, vmem_limit_bytes=KERNEL_VMEM)
        y, dx, gwqkv, gwout, sums = pl.pallas_call(
            functools.partial(body, images, tokens, dim, heads, n),
            out_shape=(
                pltpu.VMEM((num, dim), BF16),
                pltpu.VMEM((num, dim), BF16),
                pltpu.VMEM((hd, 3 * dim), BF16),
                pltpu.VMEM((hd, dim), BF16),
                pltpu.VMEM((8, LANES), F32),
            ),
            in_specs=[hbm] * 7,
            out_specs=(vmem, vmem, vmem, vmem, vmem),
            scratch_shapes=[
                pltpu.VMEM((num, dim), BF16),
                pltpu.VMEM((num, dim), BF16),
                pltpu.VMEM((dim,), F32),
                pltpu.VMEM((dim,), F32),
                pltpu.SMEM((heads,), F32),
                pltpu.VMEM((dim, 3 * dim), BF16),
                pltpu.VMEM((dim, dim), BF16),
                pltpu.VMEM((num, dim), F32),
                pltpu.VMEM((num, 1), F32),
                pltpu.VMEM((num, dim), BF16),
                pltpu.VMEM((num, dim), BF16),
                pltpu.VMEM((num, 3 * dim), BF16),
                pltpu.VMEM((num, dim), BF16),
                pltpu.VMEM((num, dim), BF16),
                pltpu.VMEM((num, 3 * dim), BF16),
                pltpu.VMEM((images, heads, G_ROWS, LANES), F32),
                pltpu.VMEM((images, n - 1, G_ROWS, LANES), F32),
                pltpu.VMEM((images, heads, P_ROWS, LANES), F32),
                pltpu.VMEM((images, n - 1, P_ROWS, LANES), F32),
                pltpu.VMEM((images, heads, BACK_ROWS, LANES), BF16),
                pltpu.VMEM((images, heads, BACK_ROWS, LANES), BF16),
                pltpu.VMEM((images, 2, 256, 256), BF16),
                pltpu.VMEM((images, 2, 256, 256), BF16),
                pltpu.VMEM((images, 8, dim), F32),
                pltpu.VMEM((images, 8, dim), F32),
                pltpu.VMEM((4, 2, 2, 2, 2, half, dim), F32),
                pltpu.VMEM((4, 2, 2, 2, half, dim), F32),
                pltpu.VMEM((4, 2, 2, 2, half, dim), F32),
                pltpu.VMEM((4, 2, half, dim), F32),
                pltpu.VMEM((4, 2, half, dim), F32),
                pltpu.VMEM((4, half, dim), F32),
                pltpu.VMEM((4, half, dim), F32),
                pltpu.VMEM((4, half, dim), F32),
                pltpu.VMEM((4, half, dim), F32),
                pltpu.VMEM((n, 8, LANES), F32),
                dma((2 * images + 5,)),
                dma((images, n - 1)), dma((images, n - 1)),
                dma((images, n - 1)), dma((images, n - 1)),
                dma((images, n - 1)), dma((images, n - 1)),
                dma((images, n - 1)), dma((images, n - 1)),
                dma((4,)), dma((4,)),
                dma((4, 2, 2)), dma((4, 2, 2)),
                dma((n - 1,)), dma((n - 1,)),
            ],
            compiler_params=params,
            name="xca_step",
        )(x_in, grad_y, ln_gain, ln_bias, w_qkv, w_out, temp_tau)
        y, dx, gwqkv, gwout, ggain, gbias, gtau = pl.pallas_call(
            functools.partial(finish, dim, heads),
            out_shape=(
                jax.ShapeDtypeStruct((num, dim), BF16),
                jax.ShapeDtypeStruct((num, dim), BF16),
                jax.ShapeDtypeStruct((hd, 3 * dim), BF16),
                jax.ShapeDtypeStruct((hd, dim), BF16),
                jax.ShapeDtypeStruct((dim,), F32),
                jax.ShapeDtypeStruct((dim,), F32),
                jax.ShapeDtypeStruct((heads,), F32),
            ),
            in_specs=[vmem] * 5,
            out_specs=(hbm, hbm, hbm, hbm, vmem, vmem, vmem),
            scratch_shapes=[dma((4,))],
            compiler_params=pltpu.CompilerParams(vmem_limit_bytes=2**20),
            name="xca_finish",
        )(y, dx, gwqkv, gwout, sums)
        return y.reshape(x_in.shape), dx.reshape(x_in.shape), gwqkv, gwout, ggain, gbias, gtau

    token_spec = P("dp", "sp", None)
    return jax.shard_map(local_step, mesh=mesh, in_specs=(token_spec, token_spec, P(), P(), P(), P(), P()), out_specs=(token_spec, token_spec, P(("dp", "sp"), None), P(("dp", "sp"), None), P("dp"), P("dp"), P("dp")), check_vma=False)
```

```python
import functools

import jax
import jax.numpy as jnp
from jax import lax
from jax.experimental import pallas as pl
from jax.experimental.pallas import tpu as pltpu
from jax.sharding import PartitionSpec as P

LN_EPS = 1e-6
MESH = pl.DeviceIdType.MESH
KERNEL_VMEM = 63713280
F32 = jnp.float32
BF16 = jnp.bfloat16
LANES = 128
G_ROWS = 24
P_ROWS = 24
BACK_ROWS = 24
STARTS = (0, 384, 768, 1152, 1408, 1536)
SPLIT = 3


def dot(a, b, ca, cb):
    return lax.dot_general(a, b, (((ca,), (cb,)), ((), ())), preferred_element_type=F32)


def roll(val, amount):
    amount = amount % LANES
    return pltpu.roll(val, amount, 1) if amount else val


def scope(name):
    return jax.named_scope(name)


def body(images, tokens, dim, heads, n,
         x_hbm, dy_hbm, gain_hbm, bias_hbm, wqkv_hbm, wout_hbm, tau_hbm,
         y_v, dx_v, gwqkv_ref, gwout_ref, sums_ref,
         x_v, dy_v, gain_v, bias_v, tau_v, wqkv_v, wout_v, xhat_v, rstd_v, du_v, u_v, ut_v, qkv_v, do_v, o_v, dqkv_v,
         g_send, g_recv, p_send, p_recv, back_a, back_g, bd_a, bd_g, c_v,
         part, pair_recv, chip_sum, x_recv, y_recv, x_send2, y_send2, x_recv2, y_recv2, ln_all,
         load_sem, g_ssem, g_rsem, p_ssem, p_rsem, a_ssem, a_rsem, d_ssem, d_rsem,
         pair_ssem, pair_rsem, st_ssem, st_rsem, ln_ssem, ln_rsem):
    hd = dim // heads
    half = hd // 2
    tiles = dim // LANES
    me = lax.axis_index("sp")
    core = lax.rem(me, 2)
    chip = me // 2
    px = lax.rem(chip, 2)
    py = chip // 2
    partner = me + 1 - 2 * core
    dev_x = me + 2 - 4 * px
    dev_y = me + 4 - 8 * py

    def dev(d):
        return {"sp": d}

    def rows(b):
        return pl.ds(pl.multiple_of(b * tokens, tokens), tokens)

    def load_x(b):
        return pltpu.make_async_copy(x_hbm.at[b], x_v.at[rows(b)], load_sem.at[b])

    def load_dy(b):
        return pltpu.make_async_copy(dy_hbm.at[b], dy_v.at[rows(b)], load_sem.at[images + b])

    load_w = [pltpu.make_async_copy(wqkv_hbm.at[:, pl.ds((i + 2) % 3 * dim, dim)], wqkv_v.at[:, pl.ds(i * dim, dim)],
                                    load_sem.at[2 * images + 5 + i]) for i in range(3)]
    load_wout = pltpu.make_async_copy(wout_hbm, wout_v, load_sem.at[2 * images])
    load_gain = pltpu.make_async_copy(gain_hbm, gain_v, load_sem.at[2 * images + 2])
    load_bias = pltpu.make_async_copy(bias_hbm, bias_v, load_sem.at[2 * images + 3])
    load_tau = pltpu.make_async_copy(tau_hbm, tau_v, load_sem.at[2 * images + 4])
    load_x(0).start()
    load_gain.start()
    load_bias.start()
    load_w[1].start()
    load_w[2].start()
    load_x(1).start()
    load_w[0].start()
    load_wout.start()
    load_dy(0).start()
    load_dy(1).start()
    load_tau.start()

    barrier = pltpu.get_barrier_semaphore()
    for off in range(1, n):
        pl.semaphore_signal(barrier, inc=1, device_id=dev(lax.rem(me + off, n)), device_id_type=MESH)

    lane = lax.broadcasted_iota(jnp.int32, (hd, LANES), 1)
    row = lax.broadcasted_iota(jnp.int32, (hd, LANES), 0)

    def pieces(h):
        base = 0 if h < SPLIT else LANES
        first = h * hd - base
        found = []
        for t in range(2):
            lo, hi = max(first, t * LANES), min(first + hd, (t + 1) * LANES)
            if lo < hi:
                found.append((t, lo - t * LANES, hi - t * LANES))
        return (0 if h < SPLIT else 1), first, found

    side = (lane[0:8, :] >= hd) & (lane[0:8, :] < hd + 16)

    def head_block(blocks, h):
        which, first, found = pieces(h)
        total = None
        for t, lo, hi in found:
            tile = blocks[which][first:first + hd, t * LANES:(t + 1) * LANES]
            tile = jnp.where((lane >= lo) & (lane < hi), tile, 0.0)
            total = tile if total is None else total + tile
        return total

    def head_row(vec, h):
        total = None
        for t in range(tiles):
            lo, hi = max(h * hd, t * LANES), min((h + 1) * hd, (t + 1) * LANES)
            if lo < hi:
                mask = (lane[0:1, :] >= lo - t * LANES) & (lane[0:1, :] < hi - t * LANES)
                tile = jnp.where(mask, vec[:, t * LANES:(t + 1) * LANES], 0.0)
                total = tile if total is None else total + tile
        return total

    def pack(val, s):
        return roll(val[0:half, :], -s) + roll(val[half:hd, :], 64 - s)

    def unpack(val):
        return jnp.concatenate([val, roll(val, 64)], axis=0)

    def beside(val, s):
        return jnp.concatenate([jnp.where(side, roll(val, hd - 16 * i - s), 0.0) for i in range(3)], axis=0)

    def exchange(send, recv, ssem, rsem, b, off):
        dst = lax.rem(me + off, n)
        return pltpu.make_async_remote_copy(
            src_ref=send.at[b, dst], dst_ref=recv.at[b, off - 1],
            send_sem=ssem.at[b, off - 1], recv_sem=rsem.at[b, off - 1],
            device_id=dev(dst), device_id_type=MESH)

    def g_copy(b, off):
        return exchange(g_send, g_recv, g_ssem, g_rsem, b, off)

    def p_copy(b, off):
        return exchange(p_send, p_recv, p_ssem, p_rsem, b, off)

    def spread(buf, ssem, rsem, b, off, src):
        return pltpu.make_async_remote_copy(
            src_ref=buf.at[b, src], dst_ref=buf.at[b, src],
            send_sem=ssem.at[b, off - 1], recv_sem=rsem.at[b, off - 1],
            device_id=dev(lax.rem(me + off, n)), device_id_type=MESH)

    def a_copy(b, off):
        return spread(back_a, a_ssem, a_rsem, b, off, me)

    def a_arrival(b, off):
        return spread(back_a, a_ssem, a_rsem, b, off, lax.rem(me + n - off, n))

    def d_copy(b, off):
        return spread(back_g, d_ssem, d_rsem, b, off, me)

    def d_arrival(b, off):
        return spread(back_g, d_ssem, d_rsem, b, off, lax.rem(me + n - off, n))

    def layer_norm(b):
        rs = rows(b)
        gain = gain_v[...].reshape(1, dim)
        bias = bias_v[...].reshape(1, dim)
        xf = x_v[rs, :].astype(F32)
        mean = jnp.mean(xf, axis=-1, keepdims=True)
        cent = xf - mean
        rstd = lax.rsqrt(jnp.mean(cent * cent, axis=-1, keepdims=True) + LN_EPS)
        xhat = cent * rstd
        xhat_v[rs, :] = xhat
        rstd_v[rs, :] = rstd
        u_v[rs, :] = (xhat * gain + bias).astype(BF16)

    def project_qk(b):
        for i in range(2):
            rs = pl.ds(b * tokens + i * (tokens // 2), tokens // 2)
            qkv_v[rs, dim:3 * dim] = dot(u_v[rs, :], wqkv_v[:, dim:3 * dim], 1, 0).astype(BF16)

    def project_v(b):
        rs = rows(b)
        qkv_v[rs, 0:dim] = dot(u_v[rs, :], wqkv_v[:, 0:dim], 1, 0).astype(BF16)

    def gram_part(b):
        rs = rows(b)
        q = qkv_v[rs, dim:2 * dim]
        k = qkv_v[rs, 2 * dim:3 * dim]
        gram = (dot(q[:, 0:256], k[:, 0:256], 0, 0), dot(q[:, 128:384], k[:, 128:384], 0, 0))
        qf = q.astype(F32)
        kf = k.astype(F32)
        ssq = jnp.sum(qf * qf, axis=0, keepdims=True)
        ssk = jnp.sum(kf * kf, axis=0, keepdims=True)
        for h in range(heads):
            s = (h * hd) % LANES
            qk = jnp.concatenate([head_row(ssq, h), head_row(ssk, h), jnp.zeros((6, LANES), F32)], axis=0)
            g_send[b, h] = pack(head_block(gram, h), s) + beside(qk, s)

    def send_g(b):
        for off in range(1, n):
            g_copy(b, off).start()

    def grad_o(b):
        rs = rows(b)
        do_v[rs, :] = dot(dy_v[rs, :], wout_v[...], 1, 1).astype(BF16)

    def prob_part(b):
        rs = rows(b)
        do = do_v[rs, :]
        v = qkv_v[rs, 0:dim]
        dprob = (dot(do[:, 0:256], v[:, 0:256], 0, 0), dot(do[:, 128:384], v[:, 128:384], 0, 0))
        for h in range(heads):
            p_send[b, h] = pack(head_block(dprob, h), (h * hd) % LANES)

    def send_p(b):
        for off in range(1, n):
            p_copy(b, off).start()

    eye = lane == row
    live = lane < hd
    live1 = live[0:1, :]

    def owner_a(b):
        tau = tau_v[me]
        with scope("wait_g"):
            for off in range(1, n):
                g_copy(b, off).wait_recv()
        total = g_send[b, me]
        for off in range(1, n):
            total = total + g_recv[b, off - 1]
        gram = unpack(total[0:half, :])
        sums = jnp.zeros((8, LANES), F32)
        for i in range(3):
            mine = (lane[0:8, :] >= 16 * i) & (lane[0:8, :] < 16 * i + 16)
            sums = jnp.where(mine, roll(total[8 * i:8 * i + 8, :], 16 * i - hd), sums)
        ssq = sums[0:1, :]
        ssk = sums[1:2, :]
        rq_col = jnp.sum(jnp.where(eye, lax.rsqrt(ssq), 0.0), axis=1, keepdims=True)
        scale = jnp.where(live, tau * rq_col * lax.rsqrt(ssk), 0.0)
        logits = jnp.where(live, gram * scale, 0.0)
        top = jnp.max(jnp.where(live, logits, -jnp.inf), axis=1, keepdims=True)
        e = jnp.where(live, jnp.exp(logits - top), 0.0)
        p = e / jnp.sum(e, axis=1, keepdims=True)
        back_a[b, me] = pack(p, 0).astype(BF16)
        for off in range(1, n):
            a_copy(b, off).start()
        return p, logits, scale, ssq, ssk

    def owner_g(b, state):
        p, logits, scale, ssq, ssk = state
        with scope("wait_p"):
            for off in range(1, n):
                p_copy(b, off).wait_recv()
        total = p_send[b, me]
        for off in range(1, n):
            total = total + p_recv[b, off - 1]
        dprob = jnp.where(live, unpack(total), 0.0).astype(BF16).astype(F32)
        glog = p * (dprob - jnp.sum(p * dprob, axis=1, keepdims=True))
        weighted = glog * logits
        w_row = jnp.sum(weighted, axis=1, keepdims=True)
        cq = -jnp.sum(jnp.where(eye, w_row, 0.0), axis=0, keepdims=True)
        cq = jnp.where(live1, cq / ssq, 0.0)
        ck = jnp.where(live1, -jnp.sum(weighted, axis=0, keepdims=True) / ssk, 0.0)
        c_rows = jnp.concatenate([cq, ck, jnp.zeros((6, LANES), F32)], axis=0)
        back_g[b, me] = (pack(glog * scale, 0) + beside(c_rows, 0)).astype(BF16)
        for off in range(1, n):
            d_copy(b, off).start()
        return jnp.sum(w_row, axis=0, keepdims=True)

    def build(b, got_of, arrival, bd, name):
        with scope(name):
            for off in range(1, n):
                arrival(b, off).wait_recv()
        found_rows = [jnp.zeros((8, LANES), F32) for _ in range(tiles)]
        for h in range(heads):
            got = got_of[b, h].astype(F32)
            which, first, found = pieces(h)
            s = first % LANES
            val = jnp.concatenate([roll(got, s), roll(got, s + 64)], axis=0)
            cols = [jnp.zeros((hd, LANES), F32) for _ in range(2)]
            for t, lo, hi in found:
                cols[t] = jnp.where((lane >= lo) & (lane < hi), val, 0.0)
            bd[b, which, first:first + hd, :] = jnp.concatenate(cols, axis=1).astype(BF16)
            for i in range(3):
                t, lo = divmod(h * hd + 16 * i, LANES)
                mine = (lane[0:8, :] >= lo) & (lane[0:8, :] < lo + 16)
                found_rows[t] = jnp.where(mine, roll(got[8 * i:8 * i + 8, :], lo - hd), found_rows[t])
        return found_rows

    def clear(bd):
        for b in range(images):
            bd[b, 0, SPLIT * hd:256, :] = jnp.zeros((256 - SPLIT * hd, 256), BF16)
            bd[b, 1, 0:SPLIT * hd - LANES, :] = jnp.zeros((SPLIT * hd - LANES, 256), BF16)

    def build_a(b):
        build(b, back_a, a_arrival, bd_a, "wait_a")

    def build_g(b):
        c_v[b] = jnp.concatenate(build(b, back_g, d_arrival, bd_g, "wait_d"), axis=1)

    def per_head(tok, mats, transposed):
        c = 1 if transposed else 0
        left = dot(tok[:, 0:256], mats[0], 1, c)
        right = dot(tok[:, 128:384], mats[1], 1, c)
        return jnp.concatenate([left[:, 0:128], left[:, 128:256] + right[:, 0:128], right[:, 128:256]], axis=1)

    def cols(c):
        return pl.ds(STARTS[c], STARTS[c + 1] - STARTS[c])

    def pair_copy(c):
        return pltpu.make_async_remote_copy(
            src_ref=part.at[:, :, 1 - core, :, :, cols(c)], dst_ref=pair_recv.at[:, :, :, :, cols(c)],
            send_sem=pair_ssem.at[c], recv_sem=pair_rsem.at[c],
            device_id=dev(partner), device_id_type=MESH)

    def stage_copies(c, stage):
        if stage == 0:
            refs = ((chip_sum.at[:, 1 - px, 0, :, cols(c)], x_recv.at[:, :, cols(c)], dev_x),
                    (chip_sum.at[1 - py, :, 1, :, cols(c)], y_recv.at[:, :, cols(c)], dev_y))
        else:
            refs = ((x_send2.at[:, cols(c)], x_recv2.at[:, cols(c)], dev_x),
                    (y_send2.at[:, cols(c)], y_recv2.at[:, cols(c)], dev_y))
        return [pltpu.make_async_remote_copy(
            src_ref=src, dst_ref=dst, send_sem=st_ssem.at[c, stage, i], recv_sem=st_rsem.at[c, stage, i],
            device_id=dev(d), device_id_type=MESH) for i, (src, dst, d) in enumerate(refs)]

    def weight_part(b, col, lhs, rhs, contract):
        value = dot(lhs, rhs, contract, 0).reshape(2, 2, 2, 2, half, dim)
        if b:
            value = value + part[:, :, :, :, :, col:col + dim]
        part[:, :, :, :, :, col:col + dim] = value

    def part_o(b):
        weight_part(b, 0, o_v[rows(b), :], dy_v[rows(b), :], 0)

    def part_qkv(b, i):
        weight_part(b, (1 + i) * dim, ut_v[:, b * tokens:(b + 1) * tokens], dqkv_v[rows(b), i * dim:(i + 1) * dim], 1)

    def rs0(c):
        pair_copy(c).start()

    def rs1(c):
        with scope("wait_pair"):
            pair_copy(c).wait_recv()
        chip_sum[:, :, :, :, cols(c)] = part[:, :, core, :, :, cols(c)] + pair_recv[:, :, :, :, cols(c)]
        for copy in stage_copies(c, 0):
            copy.start()

    def rs2(c):
        with scope("wait_st0"):
            for copy in stage_copies(c, 0):
                copy.wait_recv()
        x_send2[:, cols(c)] = chip_sum[py, 1 - px, 1, :, cols(c)] + y_recv[1 - px, :, cols(c)]
        y_send2[:, cols(c)] = chip_sum[1 - py, px, 0, :, cols(c)] + x_recv[1 - py, :, cols(c)]
        for copy in stage_copies(c, 1):
            copy.start()

    def rs3(c):
        own_a = chip_sum[py, px, 0, :, cols(c)] + x_recv[py, :, cols(c)]
        own_b = chip_sum[py, px, 1, :, cols(c)] + y_recv[px, :, cols(c)]
        with scope("wait_st1"):
            for copy in stage_copies(c, 1):
                copy.wait_recv()
        return jnp.concatenate([own_a + y_recv2[:, cols(c)], own_b + x_recv2[:, cols(c)]], axis=0).astype(BF16)

    def heads_out(b):
        rs = rows(b)
        o_v[rs, :] = per_head(qkv_v[rs, 0:dim], bd_a[b], True).astype(BF16)

    def grad_v(b):
        rs = rows(b)
        dqkv_v[rs, 0:dim] = per_head(do_v[rs, :], bd_a[b], False).astype(BF16)

    def grad_q(b):
        rs = rows(b)
        q = qkv_v[rs, dim:2 * dim]
        k = qkv_v[rs, 2 * dim:3 * dim]
        dqkv_v[rs, dim:2 * dim] = (per_head(k, bd_g[b], True) + c_v[b, 0:1, :] * q.astype(F32)).astype(BF16)

    def grad_k(b):
        rs = rows(b)
        q = qkv_v[rs, dim:2 * dim]
        k = qkv_v[rs, 2 * dim:3 * dim]
        dqkv_v[rs, 2 * dim:3 * dim] = (per_head(q, bd_g[b], False) + c_v[b, 1:2, :] * k.astype(F32)).astype(BF16)

    def out_y(b):
        rs = rows(b)
        y_v[rs, :] = (x_v[rs, :].astype(F32) + dot(o_v[rs, :], wout_v[...], 1, 0)).astype(BF16)

    def grad_u(b):
        rs = rows(b)
        du = dot(dqkv_v[rs, :], wqkv_v[...], 1, 1).astype(BF16)
        du_v[rs, :] = du
        du = du.astype(F32)
        return jnp.sum(du * xhat_v[rs, :], axis=0, keepdims=True), jnp.sum(du, axis=0, keepdims=True)

    def out_dx(b):
        rs = rows(b)
        gain = gain_v[...].reshape(1, dim)
        xhat = xhat_v[rs, :]
        a = du_v[rs, :].astype(F32) * gain
        ma = jnp.mean(a, axis=-1, keepdims=True)
        mx = jnp.mean(a * xhat, axis=-1, keepdims=True)
        dx_v[rs, :] = (dy_v[rs, :].astype(F32) + rstd_v[rs, :] * (a - ma - xhat * mx)).astype(BF16)

    with scope("phase_1"):
        clear(bd_a)
        clear(bd_g)
        load_x(0).wait()
        load_gain.wait()
        load_bias.wait()
        layer_norm(0)
        load_w[1].wait()
        load_w[2].wait()
        load_x(1).wait()
        project_qk(0)
        layer_norm(1)
        gram_part(0)
    with scope("wait_barrier"):
        pl.semaphore_wait(barrier, n - 1)
    with scope("phase_2"):
        send_g(0)
        project_qk(1)
        gram_part(1)
        send_g(1)
    with scope("phase_3"):
        load_wout.wait()
        load_dy(0).wait()
        load_w[0].wait()
        load_dy(1).wait()
        load_tau.wait()
        project_v(0)
        grad_o(0)
        prob_part(0)
        send_p(0)
        grad_o(1)
        project_v(1)
    with scope("owner_a0"):
        state0 = owner_a(0)
    with scope("phase_4"):
        prob_part(1)
        send_p(1)
    with scope("owner_a1"):
        state1 = owner_a(1)
    with scope("transpose"):
        for b in range(images):
            ut_v[:, b * tokens:(b + 1) * tokens] = u_v[rows(b), :].T
    with scope("owner_g0"):
        w0 = owner_g(0, state0)
    build_a(0)
    with scope("group1"):
        heads_out(0)
        grad_v(0)
        part_o(0)
    with scope("owner_g1"):
        w1 = owner_g(1, state1)
    build_a(1)
    with scope("group2"):
        heads_out(1)
        part_o(1)
        rs0(0)
    with scope("group3"):
        part_qkv(0, 0)
        grad_v(1)
    rs1(0)
    with scope("group3b"):
        part_qkv(1, 0)
        rs0(1)
    build_g(0)
    with scope("group4"):
        grad_q(0)
        part_qkv(0, 1)
    build_g(1)
    rs1(1)
    with scope("group5"):
        grad_q(1)
        part_qkv(1, 1)
        rs0(2)
        grad_k(0)
        grad_k(1)
        part_qkv(0, 2)
    rs1(2)
    with scope("group6"):
        part_qkv(1, 2)
        rs0(3)
        rs0(4)
    rs2(0)
    with scope("out_y"):
        out_y(0)
        out_y(1)
    rs1(3)
    rs1(4)
    rs2(1)
    with scope("group7"):
        sg0, sb0 = grad_u(0)
    rs2(2)
    with scope("group8"):
        sg1, sb1 = grad_u(1)

    sg = sg0 + sg1
    sb = sb0 + sb1
    st = jnp.where(lane[0:1, :] == me, (w0 + w1) / tau_v[me], 0.0)
    ln_rows = [val[:, t * LANES:(t + 1) * LANES] for val in (sg, sb) for t in range(tiles)]
    ln_all[me] = jnp.concatenate(ln_rows + [st, jnp.zeros((1, LANES), F32)], axis=0)

    def ln_copy(off, src):
        return pltpu.make_async_remote_copy(
            src_ref=ln_all.at[src], dst_ref=ln_all.at[src],
            send_sem=ln_ssem.at[off - 1], recv_sem=ln_rsem.at[off - 1],
            device_id=dev(lax.rem(me + off, n)), device_id_type=MESH)

    for off in range(1, n):
        ln_copy(off, me).start()

    rs2(3)
    rs2(4)
    with scope("group9"):
        out_dx(0)
        out_dx(1)
    gwout_ref[...] = rs3(0)
    gwqkv_ref[:, 2 * dim:3 * dim] = rs3(1)
    gwqkv_ref[:, 0:dim] = rs3(2)
    gwqkv_ref[:, dim:dim + 256] = rs3(3)
    gwqkv_ref[:, dim + 256:2 * dim] = rs3(4)
    with scope("wait_ln"):
        for off in range(1, n):
            ln_copy(off, lax.rem(me + n - off, n)).wait_recv()
    sums = ln_all[0]
    for d in range(1, n):
        sums = sums + ln_all[d]
    sums_ref[...] = sums

    with scope("final"):
        for b in range(images):
            for off in range(1, n):
                g_copy(b, off).wait_send()
                p_copy(b, off).wait_send()
                a_copy(b, off).wait_send()
                d_copy(b, off).wait_send()
        for c in range(5):
            pair_copy(c).wait_send()
            for stage in range(2):
                for copy in stage_copies(c, stage):
                    copy.wait_send()
        for off in range(1, n):
            ln_copy(off, me).wait_send()


def finish(dim, heads, y_v, dx_v, gwqkv_v, gwout_v, sums_v,
           y_hbm, dx_hbm, gwqkv_hbm, gwout_hbm, ggain_hbm, gbias_hbm, gtau_hbm,
           gain_v, bias_v, tau_v, sem):
    tiles = dim // LANES
    pairs = ((y_v, y_hbm), (dx_v, dx_hbm), (gwqkv_v, gwqkv_hbm), (gwout_v, gwout_hbm),
             (gain_v, ggain_hbm), (bias_v, gbias_hbm), (tau_v, gtau_hbm))
    copies = [pltpu.make_async_copy(src, dst, sem.at[i]) for i, (src, dst) in enumerate(pairs)]
    for copy in copies[:4]:
        copy.start()
    for t in range(tiles):
        gain_v[t * LANES:(t + 1) * LANES] = sums_v[t, :]
        bias_v[t * LANES:(t + 1) * LANES] = sums_v[tiles + t, :]
    tau_v[...] = sums_v[2 * tiles, 0:heads]
    for copy in copies[4:]:
        copy.start()
    for copy in copies:
        copy.wait()


def solution(mesh):
    n = mesh.shape["sp"]

    def local_step(x_in, grad_y, ln_gain, ln_bias, w_qkv, w_out, temp_tau):
        images, tokens, dim = x_in.shape
        heads = temp_tau.shape[0]
        hd = dim // heads
        half = hd // 2
        num = images * tokens
        hbm = pl.BlockSpec(memory_space=pltpu.HBM)
        vmem = pl.BlockSpec(memory_space=pltpu.VMEM)
        dma = pltpu.SemaphoreType.DMA
        params = pltpu.CompilerParams(collective_id=0, has_side_effects=True, vmem_limit_bytes=KERNEL_VMEM)
        y, dx, gwqkv, gwout, sums = pl.pallas_call(
            functools.partial(body, images, tokens, dim, heads, n),
            out_shape=(
                pltpu.VMEM((num, dim), BF16),
                pltpu.VMEM((num, dim), BF16),
                pltpu.VMEM((hd, 3 * dim), BF16),
                pltpu.VMEM((hd, dim), BF16),
                pltpu.VMEM((8, LANES), F32),
            ),
            in_specs=[hbm] * 7,
            out_specs=(vmem, vmem, vmem, vmem, vmem),
            scratch_shapes=[
                pltpu.VMEM((num, dim), BF16),
                pltpu.VMEM((num, dim), BF16),
                pltpu.VMEM((dim,), F32),
                pltpu.VMEM((dim,), F32),
                pltpu.SMEM((heads,), F32),
                pltpu.VMEM((dim, 3 * dim), BF16),
                pltpu.VMEM((dim, dim), BF16),
                pltpu.VMEM((num, dim), F32),
                pltpu.VMEM((num, 1), F32),
                pltpu.VMEM((num, dim), BF16),
                pltpu.VMEM((num, dim), BF16),
                pltpu.VMEM((dim, num), BF16),
                pltpu.VMEM((num, 3 * dim), BF16),
                pltpu.VMEM((num, dim), BF16),
                pltpu.VMEM((num, dim), BF16),
                pltpu.VMEM((num, 3 * dim), BF16),
                pltpu.VMEM((images, heads, G_ROWS, LANES), F32),
                pltpu.VMEM((images, n - 1, G_ROWS, LANES), F32),
                pltpu.VMEM((images, heads, P_ROWS, LANES), F32),
                pltpu.VMEM((images, n - 1, P_ROWS, LANES), F32),
                pltpu.VMEM((images, heads, BACK_ROWS, LANES), BF16),
                pltpu.VMEM((images, heads, BACK_ROWS, LANES), BF16),
                pltpu.VMEM((images, 2, 256, 256), BF16),
                pltpu.VMEM((images, 2, 256, 256), BF16),
                pltpu.VMEM((images, 8, dim), F32),
                pltpu.VMEM((2, 2, 2, 2, half, 4 * dim), F32),
                pltpu.VMEM((2, 2, 2, half, 4 * dim), F32),
                pltpu.VMEM((2, 2, 2, half, 4 * dim), F32),
                pltpu.VMEM((2, half, 4 * dim), F32),
                pltpu.VMEM((2, half, 4 * dim), F32),
                pltpu.VMEM((half, 4 * dim), F32),
                pltpu.VMEM((half, 4 * dim), F32),
                pltpu.VMEM((half, 4 * dim), F32),
                pltpu.VMEM((half, 4 * dim), F32),
                pltpu.VMEM((n, 8, LANES), F32),
                dma((2 * images + 8,)),
                dma((images, n - 1)), dma((images, n - 1)),
                dma((images, n - 1)), dma((images, n - 1)),
                dma((images, n - 1)), dma((images, n - 1)),
                dma((images, n - 1)), dma((images, n - 1)),
                dma((5,)), dma((5,)),
                dma((5, 2, 2)), dma((5, 2, 2)),
                dma((n - 1,)), dma((n - 1,)),
            ],
            compiler_params=params,
            name="xca_step",
        )(x_in, grad_y, ln_gain, ln_bias, w_qkv, w_out, temp_tau)
        y, dx, gwqkv, gwout, ggain, gbias, gtau = pl.pallas_call(
            functools.partial(finish, dim, heads),
            out_shape=(
                jax.ShapeDtypeStruct((num, dim), BF16),
                jax.ShapeDtypeStruct((num, dim), BF16),
                jax.ShapeDtypeStruct((hd, 3 * dim), BF16),
                jax.ShapeDtypeStruct((hd, dim), BF16),
                jax.ShapeDtypeStruct((dim,), F32),
                jax.ShapeDtypeStruct((dim,), F32),
                jax.ShapeDtypeStruct((heads,), F32),
            ),
            in_specs=[vmem] * 5,
            out_specs=(hbm,) * 7,
            scratch_shapes=[pltpu.VMEM((dim,), F32), pltpu.VMEM((dim,), F32), pltpu.VMEM((heads,), F32), dma((7,))],
            compiler_params=pltpu.CompilerParams(vmem_limit_bytes=2**20),
            name="xca_finish",
        )(y, dx, gwqkv, gwout, sums)
        return y.reshape(x_in.shape), dx.reshape(x_in.shape), gwqkv, gwout, ggain, gbias, gtau

    token_spec = P("dp", "sp", None)
    return jax.shard_map(local_step, mesh=mesh, in_specs=(token_spec, token_spec, P(), P(), P(), P(), P()), out_specs=(token_spec, token_spec, P(("dp", "sp"), None), P(("dp", "sp"), None), P("dp"), P("dp"), P("dp")), check_vma=False)
```

```python
import functools

import jax
import jax.numpy as jnp
from jax import lax
from jax.experimental import pallas as pl
from jax.experimental.pallas import tpu as pltpu
from jax.sharding import PartitionSpec as P

LN_EPS = 1e-6
MESH = pl.DeviceIdType.MESH
KERNEL_VMEM = 63713280
F32 = jnp.float32
BF16 = jnp.bfloat16
LANES = 128
G_ROWS = 24
P_ROWS = 24
BACK_ROWS = 24
STARTS = (0, 384, 768, 1152, 1408, 1536)
FAR, NEAR, PASSED = 0, 1, 2
LATE = 3
SPLIT = 3


def dot(a, b, ca, cb):
    return lax.dot_general(a, b, (((ca,), (cb,)), ((), ())), preferred_element_type=F32)


def roll(val, amount):
    amount = amount % LANES
    return pltpu.roll(val, amount, 1) if amount else val


def scope(name):
    return jax.named_scope(name)


def body(images, tokens, dim, heads, n,
         x_hbm, dy_hbm, gain_hbm, bias_hbm, wqkv_hbm, wout_hbm, tau_hbm,
         y_v, dx_v, gwqkv_ref, gwout_ref, sums_ref,
         x_v, dy_v, gain_v, bias_v, tau_v, wqkv_v, wout_v, xhat_v, rstd_v, du_v, u_v, ut_v, qkv_v, do_v, o_v, dqkv_v,
         g_send, g_recv, p_send, p_recv, back_a, back_g, bd_a, bd_g, c_v,
         part, pair_recv, chip_sum, x_recv, y_recv, x_send2, y_send2, x_recv2, y_recv2, ln_all,
         load_sem, g_ssem, g_rsem, p_ssem, p_rsem, a_ssem, a_rsem, d_ssem, d_rsem,
         pair_ssem, pair_rsem, st_ssem, far_rsem, near_rsem, passed_rsem, ln_ssem, ln_rsem):
    hd = dim // heads
    half = hd // 2
    tiles = dim // LANES
    me = lax.axis_index("sp")
    core = lax.rem(me, 2)
    chip = me // 2
    px = lax.rem(chip, 2)
    py = chip // 2
    partner = me + 1 - 2 * core
    dev_x = me + 2 - 4 * px
    dev_y = me + 4 - 8 * py

    def dev(d):
        return {"sp": d}

    def rows(b):
        return pl.ds(pl.multiple_of(b * tokens, tokens), tokens)

    def load_x(b):
        return pltpu.make_async_copy(x_hbm.at[b], x_v.at[rows(b)], load_sem.at[b])

    def load_dy(b):
        return pltpu.make_async_copy(dy_hbm.at[b], dy_v.at[rows(b)], load_sem.at[images])

    load_v = pltpu.make_async_copy(wqkv_hbm.at[:, pl.ds(2 * dim, dim)], wqkv_v.at[:, pl.ds(0, dim)], load_sem.at[images + 1])
    load_qk = pltpu.make_async_copy(wqkv_hbm.at[:, pl.ds(0, 2 * dim)], wqkv_v.at[:, pl.ds(dim, 2 * dim)], load_sem.at[images + 2])
    load_wout = pltpu.make_async_copy(wout_hbm, wout_v, load_sem.at[images + 3])
    load_gain = pltpu.make_async_copy(gain_hbm, gain_v, load_sem.at[images + 4])
    load_bias = pltpu.make_async_copy(bias_hbm, bias_v, load_sem.at[images + 5])
    load_tau = pltpu.make_async_copy(tau_hbm, tau_v, load_sem.at[images + 6])
    load_x(0).start()
    load_gain.start()
    load_bias.start()
    load_qk.start()
    load_x(1).start()
    load_v.start()
    load_wout.start()
    load_dy(0).start()
    load_dy(1).start()
    load_tau.start()

    barrier = pltpu.get_barrier_semaphore()
    for off in range(1, n):
        pl.semaphore_signal(barrier, inc=1, device_id=dev(lax.rem(me + off, n)), device_id_type=MESH)

    lane = lax.broadcasted_iota(jnp.int32, (hd, LANES), 1)
    row = lax.broadcasted_iota(jnp.int32, (hd, LANES), 0)

    def pieces(h):
        base = 0 if h < SPLIT else LANES
        first = h * hd - base
        found = []
        for t in range(2):
            lo, hi = max(first, t * LANES), min(first + hd, (t + 1) * LANES)
            if lo < hi:
                found.append((t, lo - t * LANES, hi - t * LANES))
        return (0 if h < SPLIT else 1), first, found

    side = (lane[0:8, :] >= hd) & (lane[0:8, :] < hd + 16)

    def head_block(blocks, h):
        which, first, found = pieces(h)
        total = None
        for t, lo, hi in found:
            tile = blocks[which][first:first + hd, t * LANES:(t + 1) * LANES]
            tile = jnp.where((lane >= lo) & (lane < hi), tile, 0.0)
            total = tile if total is None else total + tile
        return total

    def head_row(vec, h):
        total = None
        for t in range(tiles):
            lo, hi = max(h * hd, t * LANES), min((h + 1) * hd, (t + 1) * LANES)
            if lo < hi:
                mask = (lane[0:1, :] >= lo - t * LANES) & (lane[0:1, :] < hi - t * LANES)
                tile = jnp.where(mask, vec[:, t * LANES:(t + 1) * LANES], 0.0)
                total = tile if total is None else total + tile
        return total

    def pack(val, s):
        return roll(val[0:half, :], -s) + roll(val[half:hd, :], 64 - s)

    def unpack(val):
        return jnp.concatenate([val, roll(val, 64)], axis=0)

    def beside(val, s):
        return jnp.concatenate([jnp.where(side, roll(val, hd - 16 * i - s), 0.0) for i in range(3)], axis=0)

    def all_of(ref, ssem, rsem):
        return pltpu.make_async_remote_copy(
            src_ref=ref, dst_ref=ref, send_sem=ssem, recv_sem=rsem, device_id=dev(partner), device_id_type=MESH)

    def exchange(send, recv, ssem, rsem, b, off):
        dst = lax.rem(me + off, n)
        return pltpu.make_async_remote_copy(
            src_ref=send.at[b, dst], dst_ref=recv.at[b, off - 1],
            send_sem=ssem, recv_sem=rsem.at[b], device_id=dev(dst), device_id_type=MESH)

    def g_copy(b, off):
        return exchange(g_send, g_recv, g_ssem, g_rsem, b, off)

    def p_copy(b, off):
        return exchange(p_send, p_recv, p_ssem, p_rsem, b, off)

    def spread(buf, ssem, rsem, b, off):
        return pltpu.make_async_remote_copy(
            src_ref=buf.at[b, me], dst_ref=buf.at[b, me], send_sem=ssem, recv_sem=rsem.at[b],
            device_id=dev(lax.rem(me + off, n)), device_id_type=MESH)

    def a_copy(b, off):
        return spread(back_a, a_ssem, a_rsem, b, off)

    def d_copy(b, off):
        return spread(back_g, d_ssem, d_rsem, b, off)

    def layer_norm(b):
        rs = rows(b)
        gain = gain_v[...].reshape(1, dim)
        bias = bias_v[...].reshape(1, dim)
        xf = x_v[rs, :].astype(F32)
        mean = jnp.mean(xf, axis=-1, keepdims=True)
        cent = xf - mean
        rstd = lax.rsqrt(jnp.mean(cent * cent, axis=-1, keepdims=True) + LN_EPS)
        xhat = cent * rstd
        xhat_v[rs, :] = xhat
        rstd_v[rs, :] = rstd
        u_v[rs, :] = (xhat * gain + bias).astype(BF16)

    def project_qk(b):
        for i in range(2):
            rs = pl.ds(b * tokens + i * (tokens // 2), tokens // 2)
            qkv_v[rs, dim:3 * dim] = dot(u_v[rs, :], wqkv_v[:, dim:3 * dim], 1, 0).astype(BF16)

    def project_v(b):
        rs = rows(b)
        qkv_v[rs, 0:dim] = dot(u_v[rs, :], wqkv_v[:, 0:dim], 1, 0).astype(BF16)

    def gram_part(b):
        rs = rows(b)
        q = qkv_v[rs, dim:2 * dim]
        k = qkv_v[rs, 2 * dim:3 * dim]
        gram = (dot(q[:, 0:256], k[:, 0:256], 0, 0), dot(q[:, 128:384], k[:, 128:384], 0, 0))
        qf = q.astype(F32)
        kf = k.astype(F32)
        ssq = jnp.sum(qf * qf, axis=0, keepdims=True)
        ssk = jnp.sum(kf * kf, axis=0, keepdims=True)
        for h in range(heads):
            s = (h * hd) % LANES
            qk = jnp.concatenate([head_row(ssq, h), head_row(ssk, h), jnp.zeros((6, LANES), F32)], axis=0)
            g_send[b, h] = pack(head_block(gram, h), s) + beside(qk, s)

    def send_g(b):
        for off in range(1, n):
            g_copy(b, off).start()

    def grad_o(b):
        rs = rows(b)
        do_v[rs, :] = dot(dy_v[rs, :], wout_v[...], 1, 1).astype(BF16)

    def prob_part(b):
        rs = rows(b)
        do = do_v[rs, :]
        v = qkv_v[rs, 0:dim]
        dprob = (dot(do[:, 0:256], v[:, 0:256], 0, 0), dot(do[:, 128:384], v[:, 128:384], 0, 0))
        for h in range(heads):
            p_send[b, h] = pack(head_block(dprob, h), (h * hd) % LANES)

    def send_p(b):
        for off in range(1, n):
            p_copy(b, off).start()

    eye = lane == row
    live = lane < hd
    live1 = live[0:1, :]

    def owner_a(b):
        tau = tau_v[me]
        with scope("wait_g"):
            all_of(g_recv.at[b], g_ssem, g_rsem.at[b]).wait_recv()
        total = g_send[b, me]
        for off in range(1, n):
            total = total + g_recv[b, off - 1]
        gram = unpack(total[0:half, :])
        sums = jnp.zeros((8, LANES), F32)
        for i in range(3):
            mine = (lane[0:8, :] >= 16 * i) & (lane[0:8, :] < 16 * i + 16)
            sums = jnp.where(mine, roll(total[8 * i:8 * i + 8, :], 16 * i - hd), sums)
        ssq = sums[0:1, :]
        ssk = sums[1:2, :]
        rq_col = jnp.sum(jnp.where(eye, lax.rsqrt(ssq), 0.0), axis=1, keepdims=True)
        scale = jnp.where(live, tau * rq_col * lax.rsqrt(ssk), 0.0)
        logits = jnp.where(live, gram * scale, 0.0)
        top = jnp.max(jnp.where(live, logits, -jnp.inf), axis=1, keepdims=True)
        e = jnp.where(live, jnp.exp(logits - top), 0.0)
        p = e / jnp.sum(e, axis=1, keepdims=True)
        back_a[b, me] = pack(p, 0).astype(BF16)
        for off in range(1, n):
            a_copy(b, off).start()
        return p, logits, scale, ssq, ssk

    def owner_g(b, state):
        p, logits, scale, ssq, ssk = state
        with scope("wait_p"):
            all_of(p_recv.at[b], p_ssem, p_rsem.at[b]).wait_recv()
        total = p_send[b, me]
        for off in range(1, n):
            total = total + p_recv[b, off - 1]
        dprob = jnp.where(live, unpack(total), 0.0).astype(BF16).astype(F32)
        glog = p * (dprob - jnp.sum(p * dprob, axis=1, keepdims=True))
        weighted = glog * logits
        w_row = jnp.sum(weighted, axis=1, keepdims=True)
        cq = -jnp.sum(jnp.where(eye, w_row, 0.0), axis=0, keepdims=True)
        cq = jnp.where(live1, cq / ssq, 0.0)
        ck = jnp.where(live1, -jnp.sum(weighted, axis=0, keepdims=True) / ssk, 0.0)
        c_rows = jnp.concatenate([cq, ck, jnp.zeros((6, LANES), F32)], axis=0)
        back_g[b, me] = (pack(glog * scale, 0) + beside(c_rows, 0)).astype(BF16)
        for off in range(1, n):
            d_copy(b, off).start()
        return jnp.sum(w_row, axis=0, keepdims=True)

    def build(b, got_of, ssem, rsem, bd, name):
        with scope(name):
            all_of(got_of.at[b, pl.ds(0, n - 1)], ssem, rsem.at[b]).wait_recv()
        found_rows = [jnp.zeros((8, LANES), F32) for _ in range(tiles)]
        for h in range(heads):
            got = got_of[b, h].astype(F32)
            which, first, found = pieces(h)
            s = first % LANES
            val = jnp.concatenate([roll(got, s), roll(got, s + 64)], axis=0)
            cols = [jnp.zeros((hd, LANES), F32) for _ in range(2)]
            for t, lo, hi in found:
                cols[t] = jnp.where((lane >= lo) & (lane < hi), val, 0.0)
            bd[b, which, first:first + hd, :] = jnp.concatenate(cols, axis=1).astype(BF16)
            for i in range(3):
                t, lo = divmod(h * hd + 16 * i, LANES)
                mine = (lane[0:8, :] >= lo) & (lane[0:8, :] < lo + 16)
                found_rows[t] = jnp.where(mine, roll(got[8 * i:8 * i + 8, :], lo - hd), found_rows[t])
        return found_rows

    def clear(bd):
        for b in range(images):
            bd[b, 0, SPLIT * hd:256, :] = jnp.zeros((256 - SPLIT * hd, 256), BF16)
            bd[b, 1, 0:SPLIT * hd - LANES, :] = jnp.zeros((SPLIT * hd - LANES, 256), BF16)

    def build_a(b):
        build(b, back_a, a_ssem, a_rsem, bd_a, "wait_a")

    def build_g(b):
        c_v[b] = jnp.concatenate(build(b, back_g, d_ssem, d_rsem, bd_g, "wait_d"), axis=1)

    def per_head(tok, mats, transposed):
        c = 1 if transposed else 0
        left = dot(tok[:, 0:256], mats[0], 1, c)
        right = dot(tok[:, 128:384], mats[1], 1, c)
        return jnp.concatenate([left[:, 0:128], left[:, 128:256] + right[:, 0:128], right[:, 128:256]], axis=1)

    def cols(c):
        return pl.ds(STARTS[c], STARTS[c + 1] - STARTS[c])

    def pair_copy(c):
        return pltpu.make_async_remote_copy(
            src_ref=part.at[:, :, 1 - core, :, :, cols(c)], dst_ref=pair_recv.at[:, :, :, :, cols(c)],
            send_sem=pair_ssem, recv_sem=pair_rsem.at[c],
            device_id=dev(partner), device_id_type=MESH)

    def arrival_sem(c, stage):
        if stage == FAR:
            return far_rsem.at[c]
        return near_rsem if stage == NEAR else passed_rsem.at[0 if c < LATE else 1]

    def stage_copies(c, stage):
        if stage == FAR:
            refs = ((chip_sum.at[1 - py, 1 - px, 0, :, cols(c)], x_recv.at[1 - py, :, cols(c)], dev_x),
                    (chip_sum.at[1 - py, 1 - px, 1, :, cols(c)], y_recv.at[1 - px, :, cols(c)], dev_y))
        elif stage == NEAR:
            refs = ((chip_sum.at[py, 1 - px, 0, :, cols(c)], x_recv.at[py, :, cols(c)], dev_x),
                    (chip_sum.at[1 - py, px, 1, :, cols(c)], y_recv.at[px, :, cols(c)], dev_y))
        else:
            refs = ((x_send2.at[:, cols(c)], x_recv2.at[:, cols(c)], dev_x),
                    (y_send2.at[:, cols(c)], y_recv2.at[:, cols(c)], dev_y))
        return [pltpu.make_async_remote_copy(
            src_ref=src, dst_ref=dst, send_sem=st_ssem.at[stage], recv_sem=arrival_sem(c, stage),
            device_id=dev(d), device_id_type=MESH) for src, dst, d in refs]

    def weight_part(b, col, lhs, rhs, contract):
        value = dot(lhs, rhs, contract, 0).reshape(2, 2, 2, 2, half, dim)
        if b:
            value = value + part[:, :, :, :, :, col:col + dim]
        part[:, :, :, :, :, col:col + dim] = value

    def part_o(b):
        weight_part(b, 0, o_v[rows(b), :], dy_v[rows(b), :], 0)

    def part_qkv(b, i):
        weight_part(b, (1 + i) * dim, ut_v[:, b * tokens:(b + 1) * tokens], dqkv_v[rows(b), i * dim:(i + 1) * dim], 1)

    def rs0(c):
        pair_copy(c).start()

    def rs1(c):
        with scope("wait_pair"):
            pair_copy(c).wait_recv()
        chip_sum[:, :, :, :, cols(c)] = part[:, :, core, :, :, cols(c)] + pair_recv[:, :, :, :, cols(c)]
        for stage in (FAR, NEAR):
            for copy in stage_copies(c, stage):
                copy.start()

    def rs2(c):
        with scope("wait_st0"):
            all_of(x_recv.at[:, :, cols(c)], st_ssem.at[FAR], far_rsem.at[c]).wait_recv()
        x_send2[:, cols(c)] = chip_sum[py, 1 - px, 1, :, cols(c)] + y_recv[1 - px, :, cols(c)]
        y_send2[:, cols(c)] = chip_sum[1 - py, px, 0, :, cols(c)] + x_recv[1 - py, :, cols(c)]
        for copy in stage_copies(c, PASSED):
            copy.start()

    def rs3(lo, hi):
        own_a = chip_sum[py, px, 0, :, lo:hi] + x_recv[py, :, lo:hi]
        own_b = chip_sum[py, px, 1, :, lo:hi] + y_recv[px, :, lo:hi]
        return jnp.concatenate([own_a + y_recv2[:, lo:hi], own_b + x_recv2[:, lo:hi]], axis=0).astype(BF16)

    def heads_out(b):
        rs = rows(b)
        o_v[rs, :] = per_head(qkv_v[rs, 0:dim], bd_a[b], True).astype(BF16)

    def grad_v(b):
        rs = rows(b)
        dqkv_v[rs, 0:dim] = per_head(do_v[rs, :], bd_a[b], False).astype(BF16)

    def grad_q(b):
        rs = rows(b)
        q = qkv_v[rs, dim:2 * dim]
        k = qkv_v[rs, 2 * dim:3 * dim]
        dqkv_v[rs, dim:2 * dim] = (per_head(k, bd_g[b], True) + c_v[b, 0:1, :] * q.astype(F32)).astype(BF16)

    def grad_k(b):
        rs = rows(b)
        q = qkv_v[rs, dim:2 * dim]
        k = qkv_v[rs, 2 * dim:3 * dim]
        dqkv_v[rs, 2 * dim:3 * dim] = (per_head(q, bd_g[b], False) + c_v[b, 1:2, :] * k.astype(F32)).astype(BF16)

    def out_y(b):
        rs = rows(b)
        y_v[rs, :] = (x_v[rs, :].astype(F32) + dot(o_v[rs, :], wout_v[...], 1, 0)).astype(BF16)

    def grad_u(b, i):
        rs = pl.ds(b * tokens + i * (tokens // 2), tokens // 2)
        du = dot(dqkv_v[rs, :], wqkv_v[...], 1, 1).astype(BF16)
        du_v[rs, :] = du
        du = du.astype(F32)
        return jnp.sum(du * xhat_v[rs, :], axis=0, keepdims=True), jnp.sum(du, axis=0, keepdims=True)

    def out_dx(b):
        rs = rows(b)
        gain = gain_v[...].reshape(1, dim)
        xhat = xhat_v[rs, :]
        a = du_v[rs, :].astype(F32) * gain
        ma = jnp.mean(a, axis=-1, keepdims=True)
        mx = jnp.mean(a * xhat, axis=-1, keepdims=True)
        dx_v[rs, :] = (dy_v[rs, :].astype(F32) + rstd_v[rs, :] * (a - ma - xhat * mx)).astype(BF16)

    with scope("phase_1"):
        clear(bd_a)
        clear(bd_g)
        load_x(0).wait()
        load_gain.wait()
        load_bias.wait()
        layer_norm(0)
        load_qk.wait()
        load_x(1).wait()
        project_qk(0)
        layer_norm(1)
        gram_part(0)
    with scope("wait_barrier"):
        pl.semaphore_wait(barrier, n - 1)
    with scope("phase_2"):
        send_g(0)
        project_qk(1)
        gram_part(1)
        send_g(1)
    with scope("phase_3"):
        load_wout.wait()
        pltpu.make_async_copy(dy_v, dy_v, load_sem.at[images]).wait()
        load_v.wait()
        load_tau.wait()
        project_v(0)
        grad_o(0)
        prob_part(0)
        send_p(0)
        grad_o(1)
        project_v(1)
    with scope("owner_a0"):
        state0 = owner_a(0)
    with scope("phase_4"):
        prob_part(1)
        send_p(1)
    with scope("owner_a1"):
        state1 = owner_a(1)
    with scope("transpose"):
        for b in range(images):
            ut_v[:, b * tokens:(b + 1) * tokens] = u_v[rows(b), :].T
    with scope("owner_g0"):
        w0 = owner_g(0, state0)
    build_a(0)
    with scope("group1"):
        heads_out(0)
        grad_v(0)
        part_o(0)
    with scope("owner_g1"):
        w1 = owner_g(1, state1)
    build_a(1)
    with scope("group2"):
        heads_out(1)
        part_o(1)
        rs0(0)
    with scope("group3"):
        part_qkv(0, 0)
        grad_v(1)
    rs1(0)
    with scope("group3b"):
        part_qkv(1, 0)
        rs0(1)
    build_g(0)
    with scope("group4"):
        grad_q(0)
        part_qkv(0, 1)
    build_g(1)
    rs1(1)
    with scope("group5"):
        grad_q(1)
        part_qkv(1, 1)
        rs0(2)
        grad_k(0)
        grad_k(1)
        part_qkv(0, 2)
    rs1(2)
    rs2(0)
    with scope("group6"):
        part_qkv(1, 2)
        rs0(3)
        rs0(4)
    with scope("out_y"):
        out_y(0)
        out_y(1)
    rs1(3)
    rs1(4)
    rs2(1)
    ln_sums = []
    with scope("group7"):
        ln_sums.append(grad_u(0, 0))
        ln_sums.append(grad_u(0, 1))
        ln_sums.append(grad_u(1, 0))
    rs2(2)
    with scope("group8"):
        ln_sums.append(grad_u(1, 1))

    sg = sum(val[0] for val in ln_sums)
    sb = sum(val[1] for val in ln_sums)
    st = jnp.where(lane[0:1, :] == me, (w0 + w1) / tau_v[me], 0.0)
    ln_rows = [val[:, t * LANES:(t + 1) * LANES] for val in (sg, sb) for t in range(tiles)]
    ln_all[me] = jnp.concatenate(ln_rows + [st, jnp.zeros((1, LANES), F32)], axis=0)

    def ln_copy(off):
        return pltpu.make_async_remote_copy(
            src_ref=ln_all.at[me], dst_ref=ln_all.at[me], send_sem=ln_ssem, recv_sem=ln_rsem,
            device_id=dev(lax.rem(me + off, n)), device_id_type=MESH)

    for off in range(1, n):
        ln_copy(off).start()

    rs2(3)
    rs2(4)
    with scope("group9"):
        out_dx(0)
        out_dx(1)
    split = STARTS[LATE]
    with scope("wait_near"):
        all_of(x_recv, st_ssem.at[NEAR], near_rsem).wait_recv()
    with scope("wait_st1"):
        all_of(x_recv.at[:, :, pl.ds(0, split)], st_ssem.at[PASSED], passed_rsem.at[0]).wait_recv()
    gwout_ref[...] = rs3(0, dim)
    gwqkv_ref[:, 2 * dim:3 * dim] = rs3(dim, 2 * dim)
    gwqkv_ref[:, 0:dim] = rs3(2 * dim, 3 * dim)
    with scope("wait_ln"):
        all_of(ln_all.at[pl.ds(0, n - 1)], ln_ssem, ln_rsem).wait_recv()
    sums = ln_all[0]
    for d in range(1, n):
        sums = sums + ln_all[d]
    sums_ref[...] = sums
    with scope("wait_st1"):
        all_of(x_recv.at[:, :, pl.ds(split, 4 * dim - split)], st_ssem.at[PASSED], passed_rsem.at[1]).wait_recv()
    gwqkv_ref[:, dim:2 * dim] = rs3(3 * dim, 4 * dim)

    with scope("final"):
        all_of(g_recv, g_ssem, g_rsem.at[0]).wait_send()
        all_of(p_recv, p_ssem, p_rsem.at[0]).wait_send()
        all_of(back_a.at[:, pl.ds(0, n - 1)], a_ssem, a_rsem.at[0]).wait_send()
        all_of(back_g.at[:, pl.ds(0, n - 1)], d_ssem, d_rsem.at[0]).wait_send()
        all_of(pair_recv, pair_ssem, pair_rsem.at[0]).wait_send()
        for stage in (FAR, NEAR, PASSED):
            all_of(x_recv, st_ssem.at[stage], near_rsem).wait_send()
        all_of(ln_all.at[pl.ds(0, n - 1)], ln_ssem, ln_rsem).wait_send()


def finish(dim, heads, y_v, dx_v, gwqkv_v, gwout_v, sums_v,
           y_hbm, dx_hbm, gwqkv_hbm, gwout_hbm, ggain_hbm, gbias_hbm, gtau_hbm,
           gain_v, bias_v, tau_v, sem):
    tiles = dim // LANES
    pairs = ((y_v, y_hbm), (dx_v, dx_hbm), (gwqkv_v, gwqkv_hbm), (gwout_v, gwout_hbm),
             (gain_v, ggain_hbm), (bias_v, gbias_hbm), (tau_v, gtau_hbm))
    copies = [pltpu.make_async_copy(src, dst, sem.at[i]) for i, (src, dst) in enumerate(pairs)]
    for copy in copies[:4]:
        copy.start()
    for t in range(tiles):
        gain_v[t * LANES:(t + 1) * LANES] = sums_v[t, :]
        bias_v[t * LANES:(t + 1) * LANES] = sums_v[tiles + t, :]
    tau_v[...] = sums_v[2 * tiles, 0:heads]
    for copy in copies[4:]:
        copy.start()
    for copy in copies:
        copy.wait()


def solution(mesh):
    n = mesh.shape["sp"]

    def local_step(x_in, grad_y, ln_gain, ln_bias, w_qkv, w_out, temp_tau):
        images, tokens, dim = x_in.shape
        heads = temp_tau.shape[0]
        hd = dim // heads
        half = hd // 2
        num = images * tokens
        hbm = pl.BlockSpec(memory_space=pltpu.HBM)
        vmem = pl.BlockSpec(memory_space=pltpu.VMEM)
        dma = pltpu.SemaphoreType.DMA
        params = pltpu.CompilerParams(collective_id=0, has_side_effects=True, vmem_limit_bytes=KERNEL_VMEM)
        y, dx, gwqkv, gwout, sums = pl.pallas_call(
            functools.partial(body, images, tokens, dim, heads, n),
            out_shape=(
                pltpu.VMEM((num, dim), BF16),
                pltpu.VMEM((num, dim), BF16),
                pltpu.VMEM((hd, 3 * dim), BF16),
                pltpu.VMEM((hd, dim), BF16),
                pltpu.VMEM((8, LANES), F32),
            ),
            in_specs=[hbm] * 7,
            out_specs=(vmem, vmem, vmem, vmem, vmem),
            scratch_shapes=[
                pltpu.VMEM((num, dim), BF16),
                pltpu.VMEM((num, dim), BF16),
                pltpu.VMEM((dim,), F32),
                pltpu.VMEM((dim,), F32),
                pltpu.SMEM((heads,), F32),
                pltpu.VMEM((dim, 3 * dim), BF16),
                pltpu.VMEM((dim, dim), BF16),
                pltpu.VMEM((num, dim), F32),
                pltpu.VMEM((num, 1), F32),
                pltpu.VMEM((num, dim), BF16),
                pltpu.VMEM((num, dim), BF16),
                pltpu.VMEM((dim, num), BF16),
                pltpu.VMEM((num, 3 * dim), BF16),
                pltpu.VMEM((num, dim), BF16),
                pltpu.VMEM((num, dim), BF16),
                pltpu.VMEM((num, 3 * dim), BF16),
                pltpu.VMEM((images, heads, G_ROWS, LANES), F32),
                pltpu.VMEM((images, n - 1, G_ROWS, LANES), F32),
                pltpu.VMEM((images, heads, P_ROWS, LANES), F32),
                pltpu.VMEM((images, n - 1, P_ROWS, LANES), F32),
                pltpu.VMEM((images, heads, BACK_ROWS, LANES), BF16),
                pltpu.VMEM((images, heads, BACK_ROWS, LANES), BF16),
                pltpu.VMEM((images, 2, 256, 256), BF16),
                pltpu.VMEM((images, 2, 256, 256), BF16),
                pltpu.VMEM((images, 8, dim), F32),
                pltpu.VMEM((2, 2, 2, 2, half, 4 * dim), F32),
                pltpu.VMEM((2, 2, 2, half, 4 * dim), F32),
                pltpu.VMEM((2, 2, 2, half, 4 * dim), F32),
                pltpu.VMEM((2, half, 4 * dim), F32),
                pltpu.VMEM((2, half, 4 * dim), F32),
                pltpu.VMEM((half, 4 * dim), F32),
                pltpu.VMEM((half, 4 * dim), F32),
                pltpu.VMEM((half, 4 * dim), F32),
                pltpu.VMEM((half, 4 * dim), F32),
                pltpu.VMEM((n, 8, LANES), F32),
                dma((images + 7,)),
                dma, dma((images,)),
                dma, dma((images,)),
                dma, dma((images,)),
                dma, dma((images,)),
                dma, dma((5,)),
                dma((3,)), dma((5,)), dma, dma((2,)),
                dma, dma,
            ],
            compiler_params=params,
            name="xca_step",
        )(x_in, grad_y, ln_gain, ln_bias, w_qkv, w_out, temp_tau)
        y, dx, gwqkv, gwout, ggain, gbias, gtau = pl.pallas_call(
            functools.partial(finish, dim, heads),
            out_shape=(
                jax.ShapeDtypeStruct((num, dim), BF16),
                jax.ShapeDtypeStruct((num, dim), BF16),
                jax.ShapeDtypeStruct((hd, 3 * dim), BF16),
                jax.ShapeDtypeStruct((hd, dim), BF16),
                jax.ShapeDtypeStruct((dim,), F32),
                jax.ShapeDtypeStruct((dim,), F32),
                jax.ShapeDtypeStruct((heads,), F32),
            ),
            in_specs=[vmem] * 5,
            out_specs=(hbm,) * 7,
            scratch_shapes=[pltpu.VMEM((dim,), F32), pltpu.VMEM((dim,), F32), pltpu.VMEM((heads,), F32), dma((7,))],
            compiler_params=pltpu.CompilerParams(vmem_limit_bytes=2**20),
            name="xca_finish",
        )(y, dx, gwqkv, gwout, sums)
        return y.reshape(x_in.shape), dx.reshape(x_in.shape), gwqkv, gwout, ggain, gbias, gtau

    token_spec = P("dp", "sp", None)
    return jax.shard_map(local_step, mesh=mesh, in_specs=(token_spec, token_spec, P(), P(), P(), P(), P()), out_specs=(token_spec, token_spec, P(("dp", "sp"), None), P(("dp", "sp"), None), P("dp"), P("dp"), P("dp")), check_vma=False)
```

```python
import functools

import jax
import jax.numpy as jnp
from jax import lax
from jax.experimental import pallas as pl
from jax.experimental.pallas import tpu as pltpu
from jax.sharding import PartitionSpec as P

LN_EPS = 1e-6
MESH = pl.DeviceIdType.MESH
KERNEL_VMEM = 63713280
F32 = jnp.float32
BF16 = jnp.bfloat16
LANES = 128
G_ROWS = 24
P_ROWS = 24
BACK_ROWS = 24
STARTS = (0, 384, 768, 1152, 1408, 1536)
FAR, NEAR, PASSED = 0, 1, 2
LATE = 3
SPLIT = 3


def dot(a, b, ca, cb):
    return lax.dot_general(a, b, (((ca,), (cb,)), ((), ())), preferred_element_type=F32)


def roll(val, amount):
    amount = amount % LANES
    return pltpu.roll(val, amount, 1) if amount else val


def scope(name):
    return jax.named_scope(name)


def body(images, tokens, dim, heads, n,
         x_hbm, dy_hbm, gain_hbm, bias_hbm, wqkv_hbm, wout_hbm, tau_hbm,
         y_v, dx_v, gwqkv_ref, gwout_ref, sums_ref,
         x_v, dy_v, gain_v, bias_v, tau_v, wqkv_v, wout_v, xhat_v, rstd_v, du_v, u_v, ut_v, qkv_v, do_v, o_v, dqkv_v,
         g_send, g_recv, p_send, p_recv, back_a, back_g, bd_a, bd_g, c_v,
         part, pair_recv, chip_sum, x_recv, y_recv, x_send2, y_send2, x_recv2, y_recv2, ln_all,
         load_sem, g_ssem, g_rsem, p_ssem, p_rsem, a_ssem, a_rsem, d_ssem, d_rsem,
         pair_ssem, pair_rsem, st_ssem, far_rsem, near_rsem, passed_rsem, ln_ssem, ln_rsem):
    hd = dim // heads
    half = hd // 2
    tiles = dim // LANES
    me = lax.axis_index("sp")
    core = lax.rem(me, 2)
    chip = me // 2
    px = lax.rem(chip, 2)
    py = chip // 2
    partner = me + 1 - 2 * core
    dev_x = me + 2 - 4 * px
    dev_y = me + 4 - 8 * py

    def dev(d):
        return {"sp": d}

    def rows(b):
        return pl.ds(pl.multiple_of(b * tokens, tokens), tokens)

    def load_x(b):
        return pltpu.make_async_copy(x_hbm.at[b], x_v.at[rows(b)], load_sem.at[b])

    def load_dy(b):
        return pltpu.make_async_copy(dy_hbm.at[b], dy_v.at[rows(b)], load_sem.at[images])

    load_v = pltpu.make_async_copy(wqkv_hbm.at[:, pl.ds(2 * dim, dim)], wqkv_v.at[:, pl.ds(0, dim)], load_sem.at[images + 1])
    load_qk = pltpu.make_async_copy(wqkv_hbm.at[:, pl.ds(0, 2 * dim)], wqkv_v.at[:, pl.ds(dim, 2 * dim)], load_sem.at[images + 2])
    load_wout = pltpu.make_async_copy(wout_hbm, wout_v, load_sem.at[images + 3])
    load_gain = pltpu.make_async_copy(gain_hbm, gain_v, load_sem.at[images + 4])
    load_bias = pltpu.make_async_copy(bias_hbm, bias_v, load_sem.at[images + 5])
    load_tau = pltpu.make_async_copy(tau_hbm, tau_v, load_sem.at[images + 6])
    load_x(0).start()
    load_gain.start()
    load_bias.start()
    load_qk.start()
    load_x(1).start()
    load_v.start()
    load_wout.start()
    load_dy(0).start()
    load_dy(1).start()
    load_tau.start()

    barrier = pltpu.get_barrier_semaphore()
    for off in range(1, n):
        pl.semaphore_signal(barrier, inc=1, device_id=dev(lax.rem(me + off, n)), device_id_type=MESH)

    lane = lax.broadcasted_iota(jnp.int32, (hd, LANES), 1)
    row = lax.broadcasted_iota(jnp.int32, (hd, LANES), 0)

    def pieces(h):
        base = 0 if h < SPLIT else LANES
        first = h * hd - base
        found = []
        for t in range(2):
            lo, hi = max(first, t * LANES), min(first + hd, (t + 1) * LANES)
            if lo < hi:
                found.append((t, lo - t * LANES, hi - t * LANES))
        return (0 if h < SPLIT else 1), first, found

    side = (lane[0:8, :] >= hd) & (lane[0:8, :] < hd + 16)

    def head_block(blocks, h):
        which, first, found = pieces(h)
        total = None
        for t, lo, hi in found:
            tile = blocks[which][first:first + hd, t * LANES:(t + 1) * LANES]
            tile = jnp.where((lane >= lo) & (lane < hi), tile, 0.0)
            total = tile if total is None else total + tile
        return total

    def head_row(vec, h):
        total = None
        for t in range(tiles):
            lo, hi = max(h * hd, t * LANES), min((h + 1) * hd, (t + 1) * LANES)
            if lo < hi:
                mask = (lane[0:1, :] >= lo - t * LANES) & (lane[0:1, :] < hi - t * LANES)
                tile = jnp.where(mask, vec[:, t * LANES:(t + 1) * LANES], 0.0)
                total = tile if total is None else total + tile
        return total

    def pack(val, s):
        return roll(val[0:half, :], -s) + roll(val[half:hd, :], 64 - s)

    def unpack(val):
        return jnp.concatenate([val, roll(val, 64)], axis=0)

    def beside(val, s):
        return jnp.concatenate([jnp.where(side, roll(val, hd - 16 * i - s), 0.0) for i in range(3)], axis=0)

    def all_of(ref, ssem, rsem):
        return pltpu.make_async_remote_copy(
            src_ref=ref, dst_ref=ref, send_sem=ssem, recv_sem=rsem, device_id=dev(partner), device_id_type=MESH)

    def exchange(send, recv, ssem, rsem, b, off):
        dst = lax.rem(me + off, n)
        return pltpu.make_async_remote_copy(
            src_ref=send.at[b, dst], dst_ref=recv.at[b, off - 1],
            send_sem=ssem, recv_sem=rsem.at[b], device_id=dev(dst), device_id_type=MESH)

    def g_copy(b, off):
        return exchange(g_send, g_recv, g_ssem, g_rsem, b, off)

    def p_copy(b, off):
        return exchange(p_send, p_recv, p_ssem, p_rsem, b, off)

    def spread(buf, ssem, rsem, b, off):
        return pltpu.make_async_remote_copy(
            src_ref=buf.at[b, me], dst_ref=buf.at[b, me], send_sem=ssem, recv_sem=rsem.at[b],
            device_id=dev(lax.rem(me + off, n)), device_id_type=MESH)

    def a_copy(b, off):
        return spread(back_a, a_ssem, a_rsem, b, off)

    def d_copy(b, off):
        return spread(back_g, d_ssem, d_rsem, b, off)

    def layer_norm(b):
        rs = rows(b)
        gain = gain_v[...].reshape(1, dim)
        bias = bias_v[...].reshape(1, dim)
        xf = x_v[rs, :].astype(F32)
        mean = jnp.mean(xf, axis=-1, keepdims=True)
        cent = xf - mean
        rstd = lax.rsqrt(jnp.mean(cent * cent, axis=-1, keepdims=True) + LN_EPS)
        xhat = cent * rstd
        xhat_v[rs, :] = xhat
        rstd_v[rs, :] = rstd
        u_v[rs, :] = (xhat * gain + bias).astype(BF16)

    def project_qk(b):
        for i in range(2):
            rs = pl.ds(b * tokens + i * (tokens // 2), tokens // 2)
            qkv_v[rs, dim:3 * dim] = dot(u_v[rs, :], wqkv_v[:, dim:3 * dim], 1, 0).astype(BF16)

    def project_v(b):
        rs = rows(b)
        qkv_v[rs, 0:dim] = dot(u_v[rs, :], wqkv_v[:, 0:dim], 1, 0).astype(BF16)

    def gram_part(b):
        rs = rows(b)
        q = qkv_v[rs, dim:2 * dim]
        k = qkv_v[rs, 2 * dim:3 * dim]
        gram = (dot(q[:, 0:256], k[:, 0:256], 0, 0), dot(q[:, 128:384], k[:, 128:384], 0, 0))
        qf = q.astype(F32)
        kf = k.astype(F32)
        ssq = jnp.sum(qf * qf, axis=0, keepdims=True)
        ssk = jnp.sum(kf * kf, axis=0, keepdims=True)
        for h in range(heads):
            s = (h * hd) % LANES
            qk = jnp.concatenate([head_row(ssq, h), head_row(ssk, h), jnp.zeros((6, LANES), F32)], axis=0)
            g_send[b, h] = pack(head_block(gram, h), s) + beside(qk, s)

    def send_g(b):
        for off in range(1, n):
            g_copy(b, off).start()

    def grad_o(b):
        rs = rows(b)
        do_v[rs, :] = dot(dy_v[rs, :], wout_v[...], 1, 1).astype(BF16)

    def prob_part(b):
        rs = rows(b)
        do = do_v[rs, :]
        v = qkv_v[rs, 0:dim]
        dprob = (dot(do[:, 0:256], v[:, 0:256], 0, 0), dot(do[:, 128:384], v[:, 128:384], 0, 0))
        for h in range(heads):
            p_send[b, h] = pack(head_block(dprob, h), (h * hd) % LANES)

    def send_p(b):
        for off in range(1, n):
            p_copy(b, off).start()

    eye = lane == row
    live = lane < hd
    live1 = live[0:1, :]

    def owner_a(b):
        tau = tau_v[me]
        with scope("wait_g"):
            all_of(g_recv.at[b], g_ssem, g_rsem.at[b]).wait_recv()
        total = g_send[b, me]
        for off in range(1, n):
            total = total + g_recv[b, off - 1]
        gram = unpack(total[0:half, :])
        sums = jnp.zeros((8, LANES), F32)
        for i in range(3):
            mine = (lane[0:8, :] >= 16 * i) & (lane[0:8, :] < 16 * i + 16)
            sums = jnp.where(mine, roll(total[8 * i:8 * i + 8, :], 16 * i - hd), sums)
        ssq = sums[0:1, :]
        ssk = sums[1:2, :]
        rq_col = jnp.sum(jnp.where(eye, lax.rsqrt(ssq), 0.0), axis=1, keepdims=True)
        scale = jnp.where(live, tau * rq_col * lax.rsqrt(ssk), 0.0)
        logits = jnp.where(live, gram * scale, 0.0)
        top = jnp.max(jnp.where(live, logits, -jnp.inf), axis=1, keepdims=True)
        e = jnp.where(live, jnp.exp(logits - top), 0.0)
        p = e / jnp.sum(e, axis=1, keepdims=True)
        back_a[b, me] = pack(p, 0).astype(BF16)
        for off in range(1, n):
            a_copy(b, off).start()
        return p, logits, scale, ssq, ssk

    def owner_g(b, state):
        p, logits, scale, ssq, ssk = state
        with scope("wait_p"):
            all_of(p_recv.at[b], p_ssem, p_rsem.at[b]).wait_recv()
        total = p_send[b, me]
        for off in range(1, n):
            total = total + p_recv[b, off - 1]
        dprob = jnp.where(live, unpack(total), 0.0).astype(BF16).astype(F32)
        glog = p * (dprob - jnp.sum(p * dprob, axis=1, keepdims=True))
        weighted = glog * logits
        w_row = jnp.sum(weighted, axis=1, keepdims=True)
        cq = -jnp.sum(jnp.where(eye, w_row, 0.0), axis=0, keepdims=True)
        cq = jnp.where(live1, cq / ssq, 0.0)
        ck = jnp.where(live1, -jnp.sum(weighted, axis=0, keepdims=True) / ssk, 0.0)
        c_rows = jnp.concatenate([cq, ck, jnp.zeros((6, LANES), F32)], axis=0)
        back_g[b, me] = (pack(glog * scale, 0) + beside(c_rows, 0)).astype(BF16)
        for off in range(1, n):
            d_copy(b, off).start()
        return jnp.sum(w_row, axis=0, keepdims=True)

    def build(b, got_of, ssem, rsem, bd, name):
        with scope(name):
            all_of(got_of.at[b, pl.ds(0, n - 1)], ssem, rsem.at[b]).wait_recv()
        found_rows = [jnp.zeros((8, LANES), F32) for _ in range(tiles)]
        for h in range(heads):
            got = got_of[b, h].astype(F32)
            which, first, found = pieces(h)
            s = first % LANES
            val = jnp.concatenate([roll(got, s), roll(got, s + 64)], axis=0)
            cols = [jnp.zeros((hd, LANES), F32) for _ in range(2)]
            for t, lo, hi in found:
                cols[t] = jnp.where((lane >= lo) & (lane < hi), val, 0.0)
            bd[b, which, first:first + hd, :] = jnp.concatenate(cols, axis=1).astype(BF16)
            for i in range(3):
                t, lo = divmod(h * hd + 16 * i, LANES)
                mine = (lane[0:8, :] >= lo) & (lane[0:8, :] < lo + 16)
                found_rows[t] = jnp.where(mine, roll(got[8 * i:8 * i + 8, :], lo - hd), found_rows[t])
        return found_rows

    def clear(bd):
        for b in range(images):
            bd[b, 0, SPLIT * hd:256, :] = jnp.zeros((256 - SPLIT * hd, 256), BF16)
            bd[b, 1, 0:SPLIT * hd - LANES, :] = jnp.zeros((SPLIT * hd - LANES, 256), BF16)

    def build_a(b):
        build(b, back_a, a_ssem, a_rsem, bd_a, "wait_a")

    def build_g(b):
        c_v[b] = jnp.concatenate(build(b, back_g, d_ssem, d_rsem, bd_g, "wait_d"), axis=1)

    def per_head(tok, mats, transposed):
        c = 1 if transposed else 0
        left = dot(tok[:, 0:256], mats[0], 1, c)
        right = dot(tok[:, 128:384], mats[1], 1, c)
        return jnp.concatenate([left[:, 0:128], left[:, 128:256] + right[:, 0:128], right[:, 128:256]], axis=1)

    def cols(c):
        return pl.ds(STARTS[c], STARTS[c + 1] - STARTS[c])

    def pair_copy(c):
        return pltpu.make_async_remote_copy(
            src_ref=part.at[:, :, 1 - core, :, :, cols(c)], dst_ref=pair_recv.at[:, :, :, :, cols(c)],
            send_sem=pair_ssem, recv_sem=pair_rsem.at[c],
            device_id=dev(partner), device_id_type=MESH)

    def arrival_sem(c, stage):
        if stage == FAR:
            return far_rsem.at[c]
        return near_rsem if stage == NEAR else passed_rsem.at[0 if c < LATE else 1]

    def stage_copies(c, stage):
        if stage == FAR:
            refs = ((chip_sum.at[1 - py, 1 - px, 0, :, cols(c)], x_recv.at[1 - py, :, cols(c)], dev_x),
                    (chip_sum.at[1 - py, 1 - px, 1, :, cols(c)], y_recv.at[1 - px, :, cols(c)], dev_y))
        elif stage == NEAR:
            refs = ((chip_sum.at[py, 1 - px, 0, :, cols(c)], x_recv.at[py, :, cols(c)], dev_x),
                    (chip_sum.at[1 - py, px, 1, :, cols(c)], y_recv.at[px, :, cols(c)], dev_y))
        else:
            refs = ((x_send2.at[:, cols(c)], x_recv2.at[:, cols(c)], dev_x),
                    (y_send2.at[:, cols(c)], y_recv2.at[:, cols(c)], dev_y))
        return [pltpu.make_async_remote_copy(
            src_ref=src, dst_ref=dst, send_sem=st_ssem.at[stage], recv_sem=arrival_sem(c, stage),
            device_id=dev(d), device_id_type=MESH) for src, dst, d in refs]

    def weight_part(b, col, lhs, rhs, contract):
        value = dot(lhs, rhs, contract, 0).reshape(2, 2, 2, 2, half, dim)
        if b:
            value = value + part[:, :, :, :, :, col:col + dim]
        part[:, :, :, :, :, col:col + dim] = value

    def part_o(b):
        weight_part(b, 0, o_v[rows(b), :], dy_v[rows(b), :], 0)

    def part_qkv(b, i):
        weight_part(b, (1 + i) * dim, ut_v[:, b * tokens:(b + 1) * tokens], dqkv_v[rows(b), i * dim:(i + 1) * dim], 1)

    def rs0(c):
        pair_copy(c).start()

    def rs1(*chunks):
        for c in chunks:
            with scope("wait_pair"):
                pair_copy(c).wait_recv()
            chip_sum[:, :, :, :, cols(c)] = part[:, :, core, :, :, cols(c)] + pair_recv[:, :, :, :, cols(c)]
            for copy in stage_copies(c, FAR):
                copy.start()
        for c in chunks:
            for copy in stage_copies(c, NEAR):
                copy.start()

    def rs2(c):
        with scope("wait_st0"):
            all_of(x_recv.at[:, :, cols(c)], st_ssem.at[FAR], far_rsem.at[c]).wait_recv()
        x_send2[:, cols(c)] = chip_sum[py, 1 - px, 1, :, cols(c)] + y_recv[1 - px, :, cols(c)]
        y_send2[:, cols(c)] = chip_sum[1 - py, px, 0, :, cols(c)] + x_recv[1 - py, :, cols(c)]
        for copy in stage_copies(c, PASSED):
            copy.start()

    def rs3(lo, hi):
        own_a = chip_sum[py, px, 0, :, lo:hi] + x_recv[py, :, lo:hi]
        own_b = chip_sum[py, px, 1, :, lo:hi] + y_recv[px, :, lo:hi]
        return jnp.concatenate([own_a + y_recv2[:, lo:hi], own_b + x_recv2[:, lo:hi]], axis=0).astype(BF16)

    def heads_out(b):
        rs = rows(b)
        o_v[rs, :] = per_head(qkv_v[rs, 0:dim], bd_a[b], True).astype(BF16)

    def grad_v(b):
        rs = rows(b)
        dqkv_v[rs, 0:dim] = per_head(do_v[rs, :], bd_a[b], False).astype(BF16)

    def grad_q(b):
        rs = rows(b)
        q = qkv_v[rs, dim:2 * dim]
        k = qkv_v[rs, 2 * dim:3 * dim]
        dqkv_v[rs, dim:2 * dim] = (per_head(k, bd_g[b], True) + c_v[b, 0:1, :] * q.astype(F32)).astype(BF16)

    def grad_k(b):
        rs = rows(b)
        q = qkv_v[rs, dim:2 * dim]
        k = qkv_v[rs, 2 * dim:3 * dim]
        dqkv_v[rs, 2 * dim:3 * dim] = (per_head(q, bd_g[b], False) + c_v[b, 1:2, :] * k.astype(F32)).astype(BF16)

    def out_y(b):
        rs = rows(b)
        y_v[rs, :] = (x_v[rs, :].astype(F32) + dot(o_v[rs, :], wout_v[...], 1, 0)).astype(BF16)

    def grad_u(b, i):
        rs = pl.ds(b * tokens + i * (tokens // 2), tokens // 2)
        du = dot(dqkv_v[rs, :], wqkv_v[...], 1, 1).astype(BF16)
        du_v[rs, :] = du
        du = du.astype(F32)
        return jnp.sum(du * xhat_v[rs, :], axis=0, keepdims=True), jnp.sum(du, axis=0, keepdims=True)

    def out_dx(b):
        rs = rows(b)
        gain = gain_v[...].reshape(1, dim)
        xhat = xhat_v[rs, :]
        a = du_v[rs, :].astype(F32) * gain
        ma = jnp.mean(a, axis=-1, keepdims=True)
        mx = jnp.mean(a * xhat, axis=-1, keepdims=True)
        dx_v[rs, :] = (dy_v[rs, :].astype(F32) + rstd_v[rs, :] * (a - ma - xhat * mx)).astype(BF16)

    with scope("phase_1"):
        clear(bd_a)
        clear(bd_g)
        load_x(0).wait()
        load_gain.wait()
        load_bias.wait()
        layer_norm(0)
        load_qk.wait()
        load_x(1).wait()
        project_qk(0)
        layer_norm(1)
        gram_part(0)
    with scope("wait_barrier"):
        pl.semaphore_wait(barrier, n - 1)
    with scope("phase_2"):
        send_g(0)
        project_qk(1)
        gram_part(1)
        send_g(1)
    with scope("phase_3"):
        load_wout.wait()
        pltpu.make_async_copy(dy_v, dy_v, load_sem.at[images]).wait()
        load_v.wait()
        load_tau.wait()
        project_v(0)
        grad_o(0)
        prob_part(0)
        send_p(0)
        grad_o(1)
        project_v(1)
    with scope("owner_a0"):
        state0 = owner_a(0)
    with scope("phase_4"):
        prob_part(1)
        send_p(1)
    with scope("owner_a1"):
        state1 = owner_a(1)
    with scope("transpose"):
        for b in range(images):
            ut_v[:, b * tokens:(b + 1) * tokens] = u_v[rows(b), :].T
    with scope("owner_g0"):
        w0 = owner_g(0, state0)
    build_a(0)
    with scope("group1"):
        heads_out(0)
        grad_v(0)
        part_o(0)
    with scope("owner_g1"):
        w1 = owner_g(1, state1)
    build_a(1)
    with scope("group2"):
        heads_out(1)
        part_o(1)
        rs0(0)
    with scope("group3"):
        part_qkv(0, 0)
        grad_v(1)
        part_qkv(1, 0)
        rs0(1)
    rs1(0)
    build_g(0)
    with scope("group4"):
        grad_q(0)
        part_qkv(0, 1)
        grad_k(0)
    build_g(1)
    with scope("group4b"):
        grad_q(1)
    rs1(1)
    with scope("group5"):
        part_qkv(1, 1)
        rs0(2)
        grad_k(1)
        part_qkv(0, 2)
    rs2(0)
    with scope("group6"):
        part_qkv(1, 2)
        rs0(3)
        rs0(4)
    rs1(2)
    ln_sums = []
    with scope("group7"):
        out_y(0)
        out_y(1)
    rs1(3, 4)
    rs2(1)
    with scope("group8"):
        ln_sums.append(grad_u(0, 0))
        ln_sums.append(grad_u(0, 1))
        ln_sums.append(grad_u(1, 0))
    rs2(2)
    with scope("group8b"):
        ln_sums.append(grad_u(1, 1))

    sg = sum(val[0] for val in ln_sums)
    sb = sum(val[1] for val in ln_sums)
    st = jnp.where(lane[0:1, :] == me, (w0 + w1) / tau_v[me], 0.0)
    ln_rows = [val[:, t * LANES:(t + 1) * LANES] for val in (sg, sb) for t in range(tiles)]
    ln_all[me] = jnp.concatenate(ln_rows + [st, jnp.zeros((1, LANES), F32)], axis=0)

    def ln_copy(off):
        return pltpu.make_async_remote_copy(
            src_ref=ln_all.at[me], dst_ref=ln_all.at[me], send_sem=ln_ssem, recv_sem=ln_rsem,
            device_id=dev(lax.rem(me + off, n)), device_id_type=MESH)

    for off in range(1, n):
        ln_copy(off).start()

    rs2(3)
    rs2(4)
    with scope("group9"):
        out_dx(0)
        out_dx(1)
    split = STARTS[LATE]
    with scope("wait_near"):
        all_of(x_recv, st_ssem.at[NEAR], near_rsem).wait_recv()
    with scope("wait_st1"):
        all_of(x_recv.at[:, :, pl.ds(0, split)], st_ssem.at[PASSED], passed_rsem.at[0]).wait_recv()
    gwout_ref[...] = rs3(0, dim)
    gwqkv_ref[:, 2 * dim:3 * dim] = rs3(dim, 2 * dim)
    gwqkv_ref[:, 0:dim] = rs3(2 * dim, 3 * dim)
    with scope("wait_ln"):
        all_of(ln_all.at[pl.ds(0, n - 1)], ln_ssem, ln_rsem).wait_recv()
    sums = ln_all[0]
    for d in range(1, n):
        sums = sums + ln_all[d]
    sums_ref[...] = sums
    with scope("wait_st1"):
        all_of(x_recv.at[:, :, pl.ds(split, 4 * dim - split)], st_ssem.at[PASSED], passed_rsem.at[1]).wait_recv()
    gwqkv_ref[:, dim:2 * dim] = rs3(3 * dim, 4 * dim)

    with scope("final"):
        all_of(g_recv, g_ssem, g_rsem.at[0]).wait_send()
        all_of(p_recv, p_ssem, p_rsem.at[0]).wait_send()
        all_of(back_a.at[:, pl.ds(0, n - 1)], a_ssem, a_rsem.at[0]).wait_send()
        all_of(back_g.at[:, pl.ds(0, n - 1)], d_ssem, d_rsem.at[0]).wait_send()
        all_of(pair_recv, pair_ssem, pair_rsem.at[0]).wait_send()
        for stage in (FAR, NEAR, PASSED):
            all_of(x_recv, st_ssem.at[stage], near_rsem).wait_send()
        all_of(ln_all.at[pl.ds(0, n - 1)], ln_ssem, ln_rsem).wait_send()


def finish(dim, heads, y_v, dx_v, gwqkv_v, gwout_v, sums_v,
           y_hbm, dx_hbm, gwqkv_hbm, gwout_hbm, ggain_hbm, gbias_hbm, gtau_hbm,
           gain_v, bias_v, tau_v, sem):
    tiles = dim // LANES
    pairs = ((y_v, y_hbm), (dx_v, dx_hbm), (gwqkv_v, gwqkv_hbm), (gwout_v, gwout_hbm),
             (gain_v, ggain_hbm), (bias_v, gbias_hbm), (tau_v, gtau_hbm))
    copies = [pltpu.make_async_copy(src, dst, sem.at[i]) for i, (src, dst) in enumerate(pairs)]
    for copy in copies[:4]:
        copy.start()
    for t in range(tiles):
        gain_v[t * LANES:(t + 1) * LANES] = sums_v[t, :]
        bias_v[t * LANES:(t + 1) * LANES] = sums_v[tiles + t, :]
    tau_v[...] = sums_v[2 * tiles, 0:heads]
    for copy in copies[4:]:
        copy.start()
    for copy in copies:
        copy.wait()


def solution(mesh):
    n = mesh.shape["sp"]

    def local_step(x_in, grad_y, ln_gain, ln_bias, w_qkv, w_out, temp_tau):
        images, tokens, dim = x_in.shape
        heads = temp_tau.shape[0]
        hd = dim // heads
        half = hd // 2
        num = images * tokens
        hbm = pl.BlockSpec(memory_space=pltpu.HBM)
        vmem = pl.BlockSpec(memory_space=pltpu.VMEM)
        dma = pltpu.SemaphoreType.DMA
        params = pltpu.CompilerParams(collective_id=0, has_side_effects=True, vmem_limit_bytes=KERNEL_VMEM)
        y, dx, gwqkv, gwout, sums = pl.pallas_call(
            functools.partial(body, images, tokens, dim, heads, n),
            out_shape=(
                pltpu.VMEM((num, dim), BF16),
                pltpu.VMEM((num, dim), BF16),
                pltpu.VMEM((hd, 3 * dim), BF16),
                pltpu.VMEM((hd, dim), BF16),
                pltpu.VMEM((8, LANES), F32),
            ),
            in_specs=[hbm] * 7,
            out_specs=(vmem, vmem, vmem, vmem, vmem),
            scratch_shapes=[
                pltpu.VMEM((num, dim), BF16),
                pltpu.VMEM((num, dim), BF16),
                pltpu.VMEM((dim,), F32),
                pltpu.VMEM((dim,), F32),
                pltpu.SMEM((heads,), F32),
                pltpu.VMEM((dim, 3 * dim), BF16),
                pltpu.VMEM((dim, dim), BF16),
                pltpu.VMEM((num, dim), F32),
                pltpu.VMEM((num, 1), F32),
                pltpu.VMEM((num, dim), BF16),
                pltpu.VMEM((num, dim), BF16),
                pltpu.VMEM((dim, num), BF16),
                pltpu.VMEM((num, 3 * dim), BF16),
                pltpu.VMEM((num, dim), BF16),
                pltpu.VMEM((num, dim), BF16),
                pltpu.VMEM((num, 3 * dim), BF16),
                pltpu.VMEM((images, heads, G_ROWS, LANES), F32),
                pltpu.VMEM((images, n - 1, G_ROWS, LANES), F32),
                pltpu.VMEM((images, heads, P_ROWS, LANES), F32),
                pltpu.VMEM((images, n - 1, P_ROWS, LANES), F32),
                pltpu.VMEM((images, heads, BACK_ROWS, LANES), BF16),
                pltpu.VMEM((images, heads, BACK_ROWS, LANES), BF16),
                pltpu.VMEM((images, 2, 256, 256), BF16),
                pltpu.VMEM((images, 2, 256, 256), BF16),
                pltpu.VMEM((images, 8, dim), F32),
                pltpu.VMEM((2, 2, 2, 2, half, 4 * dim), F32),
                pltpu.VMEM((2, 2, 2, half, 4 * dim), F32),
                pltpu.VMEM((2, 2, 2, half, 4 * dim), F32),
                pltpu.VMEM((2, half, 4 * dim), F32),
                pltpu.VMEM((2, half, 4 * dim), F32),
                pltpu.VMEM((half, 4 * dim), F32),
                pltpu.VMEM((half, 4 * dim), F32),
                pltpu.VMEM((half, 4 * dim), F32),
                pltpu.VMEM((half, 4 * dim), F32),
                pltpu.VMEM((n, 8, LANES), F32),
                dma((images + 7,)),
                dma, dma((images,)),
                dma, dma((images,)),
                dma, dma((images,)),
                dma, dma((images,)),
                dma, dma((5,)),
                dma((3,)), dma((5,)), dma, dma((2,)),
                dma, dma,
            ],
            compiler_params=params,
            name="xca_step",
        )(x_in, grad_y, ln_gain, ln_bias, w_qkv, w_out, temp_tau)
        y, dx, gwqkv, gwout, ggain, gbias, gtau = pl.pallas_call(
            functools.partial(finish, dim, heads),
            out_shape=(
                jax.ShapeDtypeStruct((num, dim), BF16),
                jax.ShapeDtypeStruct((num, dim), BF16),
                jax.ShapeDtypeStruct((hd, 3 * dim), BF16),
                jax.ShapeDtypeStruct((hd, dim), BF16),
                jax.ShapeDtypeStruct((dim,), F32),
                jax.ShapeDtypeStruct((dim,), F32),
                jax.ShapeDtypeStruct((heads,), F32),
            ),
            in_specs=[vmem] * 5,
            out_specs=(hbm,) * 7,
            scratch_shapes=[pltpu.VMEM((dim,), F32), pltpu.VMEM((dim,), F32), pltpu.VMEM((heads,), F32), dma((7,))],
            compiler_params=pltpu.CompilerParams(vmem_limit_bytes=2**20),
            name="xca_finish",
        )(y, dx, gwqkv, gwout, sums)
        return y.reshape(x_in.shape), dx.reshape(x_in.shape), gwqkv, gwout, ggain, gbias, gtau

    token_spec = P("dp", "sp", None)
    return jax.shard_map(local_step, mesh=mesh, in_specs=(token_spec, token_spec, P(), P(), P(), P(), P()), out_specs=(token_spec, token_spec, P(("dp", "sp"), None), P(("dp", "sp"), None), P("dp"), P("dp"), P("dp")), check_vma=False)
```

```python
import functools

import jax
import jax.numpy as jnp
from jax import lax
from jax.experimental import pallas as pl
from jax.experimental.pallas import tpu as pltpu
from jax.sharding import PartitionSpec as P

LN_EPS = 1e-6
MESH = pl.DeviceIdType.MESH
KERNEL_VMEM = 63713280
F32 = jnp.float32
BF16 = jnp.bfloat16
LANES = 128
G_ROWS = 24
P_ROWS = 24
BACK_ROWS = 24
STARTS = (0, 384, 768, 1152, 1408, 1536)
FAR, NEAR, PASSED = 0, 1, 2
LATE = 3
SPLIT = 3


def dot(a, b, ca, cb):
    return lax.dot_general(a, b, (((ca,), (cb,)), ((), ())), preferred_element_type=F32)


def roll(val, amount):
    amount = amount % LANES
    return pltpu.roll(val, amount, 1) if amount else val


def scope(name):
    return jax.named_scope(name)


def body(images, tokens, dim, heads, n,
         x_hbm, dy_hbm, gain_hbm, bias_hbm, wqkv_hbm, wout_hbm, tau_hbm,
         y_v, dx_v, gwqkv_ref, gwout_ref, sums_ref,
         x_v, dy_v, gain_v, bias_v, tau_v, wqkv_v, wout_v, xhat_v, rstd_v, du_v, u_v, ut_v, qkv_v, do_v, o_v, dqkv_v,
         g_send, g_recv, p_send, p_recv, back_a, back_g, bd_a, bd_g, c_v,
         part, pair_recv, chip_sum, x_recv, y_recv, x_send2, y_send2, x_recv2, y_recv2, ln_all,
         load_sem, g_ssem, g_rsem, p_ssem, p_rsem, a_ssem, a_rsem, d_ssem, d_rsem,
         pair_ssem, pair_rsem, st_ssem, far_rsem, near_rsem, passed_rsem, ln_ssem, ln_rsem):
    hd = dim // heads
    half = hd // 2
    tiles = dim // LANES
    me = lax.axis_index("sp")
    core = lax.rem(me, 2)
    chip = me // 2
    px = lax.rem(chip, 2)
    py = chip // 2
    partner = me + 1 - 2 * core
    dev_x = me + 2 - 4 * px
    dev_y = me + 4 - 8 * py

    dev_d = 6 + 2 * core - me
    other = 1 - 2 * core
    peers = (dev_d, dev_d + other, dev_x, dev_y, dev_x + other, dev_y + other, partner)

    def dev(d):
        return {"sp": d}

    def rows(b):
        return pl.ds(pl.multiple_of(b * tokens, tokens), tokens)

    def load_x(b):
        return pltpu.make_async_copy(x_hbm.at[b], x_v.at[rows(b)], load_sem.at[b])

    def load_dy(b):
        return pltpu.make_async_copy(dy_hbm.at[b], dy_v.at[rows(b)], load_sem.at[images])

    load_v = pltpu.make_async_copy(wqkv_hbm.at[:, pl.ds(2 * dim, dim)], wqkv_v.at[:, pl.ds(0, dim)], load_sem.at[images + 1])
    load_qk = pltpu.make_async_copy(wqkv_hbm.at[:, pl.ds(0, 2 * dim)], wqkv_v.at[:, pl.ds(dim, 2 * dim)], load_sem.at[images + 2])
    load_wout = pltpu.make_async_copy(wout_hbm, wout_v, load_sem.at[images + 3])
    load_gain = pltpu.make_async_copy(gain_hbm, gain_v, load_sem.at[images + 4])
    load_bias = pltpu.make_async_copy(bias_hbm, bias_v, load_sem.at[images + 5])
    load_tau = pltpu.make_async_copy(tau_hbm, tau_v, load_sem.at[images + 6])
    load_x(0).start()
    load_gain.start()
    load_bias.start()
    load_qk.start()
    load_x(1).start()
    load_v.start()
    load_wout.start()
    load_dy(0).start()
    load_dy(1).start()
    load_tau.start()

    barrier = pltpu.get_barrier_semaphore()
    for off in range(1, n):
        pl.semaphore_signal(barrier, inc=1, device_id=dev(peers[off - 1]), device_id_type=MESH)

    lane = lax.broadcasted_iota(jnp.int32, (hd, LANES), 1)
    row = lax.broadcasted_iota(jnp.int32, (hd, LANES), 0)

    def pieces(h):
        base = 0 if h < SPLIT else LANES
        first = h * hd - base
        found = []
        for t in range(2):
            lo, hi = max(first, t * LANES), min(first + hd, (t + 1) * LANES)
            if lo < hi:
                found.append((t, lo - t * LANES, hi - t * LANES))
        return (0 if h < SPLIT else 1), first, found

    side = (lane[0:8, :] >= hd) & (lane[0:8, :] < hd + 16)

    def head_block(blocks, h):
        which, first, found = pieces(h)
        total = None
        for t, lo, hi in found:
            tile = blocks[which][first:first + hd, t * LANES:(t + 1) * LANES]
            tile = jnp.where((lane >= lo) & (lane < hi), tile, 0.0)
            total = tile if total is None else total + tile
        return total

    def head_row(vec, h):
        total = None
        for t in range(tiles):
            lo, hi = max(h * hd, t * LANES), min((h + 1) * hd, (t + 1) * LANES)
            if lo < hi:
                mask = (lane[0:1, :] >= lo - t * LANES) & (lane[0:1, :] < hi - t * LANES)
                tile = jnp.where(mask, vec[:, t * LANES:(t + 1) * LANES], 0.0)
                total = tile if total is None else total + tile
        return total

    def pack(val, s):
        return roll(val[0:half, :], -s) + roll(val[half:hd, :], 64 - s)

    def unpack(val):
        return jnp.concatenate([val, roll(val, 64)], axis=0)

    def beside(val, s):
        return jnp.concatenate([jnp.where(side, roll(val, hd - 16 * i - s), 0.0) for i in range(3)], axis=0)

    def all_of(ref, ssem, rsem):
        return pltpu.make_async_remote_copy(
            src_ref=ref, dst_ref=ref, send_sem=ssem, recv_sem=rsem, device_id=dev(partner), device_id_type=MESH)

    def exchange(send, recv, ssem, rsem, b, off):
        dst = peers[off - 1]
        return pltpu.make_async_remote_copy(
            src_ref=send.at[b, dst], dst_ref=recv.at[b, off - 1],
            send_sem=ssem, recv_sem=rsem.at[b], device_id=dev(dst), device_id_type=MESH)

    def g_copy(b, off):
        return exchange(g_send, g_recv, g_ssem, g_rsem, b, off)

    def p_copy(b, off):
        return exchange(p_send, p_recv, p_ssem, p_rsem, b, off)

    def spread(buf, ssem, rsem, b, off):
        return pltpu.make_async_remote_copy(
            src_ref=buf.at[b, me], dst_ref=buf.at[b, me], send_sem=ssem, recv_sem=rsem.at[b],
            device_id=dev(peers[off - 1]), device_id_type=MESH)

    def a_copy(b, off):
        return spread(back_a, a_ssem, a_rsem, b, off)

    def d_copy(b, off):
        return spread(back_g, d_ssem, d_rsem, b, off)

    def layer_norm(b):
        rs = rows(b)
        gain = gain_v[...].reshape(1, dim)
        bias = bias_v[...].reshape(1, dim)
        xf = x_v[rs, :].astype(F32)
        mean = jnp.mean(xf, axis=-1, keepdims=True)
        cent = xf - mean
        rstd = lax.rsqrt(jnp.mean(cent * cent, axis=-1, keepdims=True) + LN_EPS)
        xhat = cent * rstd
        xhat_v[rs, :] = xhat
        rstd_v[rs, :] = rstd
        u_v[rs, :] = (xhat * gain + bias).astype(BF16)

    def project_qk(b):
        for i in range(2):
            rs = pl.ds(b * tokens + i * (tokens // 2), tokens // 2)
            qkv_v[rs, dim:3 * dim] = dot(u_v[rs, :], wqkv_v[:, dim:3 * dim], 1, 0).astype(BF16)

    def project_v(b):
        rs = rows(b)
        qkv_v[rs, 0:dim] = dot(u_v[rs, :], wqkv_v[:, 0:dim], 1, 0).astype(BF16)

    def gram_part(b):
        rs = rows(b)
        q = qkv_v[rs, dim:2 * dim]
        k = qkv_v[rs, 2 * dim:3 * dim]
        gram = (dot(q[:, 0:256], k[:, 0:256], 0, 0), dot(q[:, 128:384], k[:, 128:384], 0, 0))
        qf = q.astype(F32)
        kf = k.astype(F32)
        ssq = jnp.sum(qf * qf, axis=0, keepdims=True)
        ssk = jnp.sum(kf * kf, axis=0, keepdims=True)
        for h in range(heads):
            s = (h * hd) % LANES
            qk = jnp.concatenate([head_row(ssq, h), head_row(ssk, h), jnp.zeros((6, LANES), F32)], axis=0)
            g_send[b, h] = pack(head_block(gram, h), s) + beside(qk, s)

    def send_g(b):
        for off in range(1, n):
            g_copy(b, off).start()

    def grad_o(b):
        rs = rows(b)
        do_v[rs, :] = dot(dy_v[rs, :], wout_v[...], 1, 1).astype(BF16)

    def prob_part(b):
        rs = rows(b)
        do = do_v[rs, :]
        v = qkv_v[rs, 0:dim]
        dprob = (dot(do[:, 0:256], v[:, 0:256], 0, 0), dot(do[:, 128:384], v[:, 128:384], 0, 0))
        for h in range(heads):
            p_send[b, h] = pack(head_block(dprob, h), (h * hd) % LANES)

    def send_p(b):
        for off in range(1, n):
            p_copy(b, off).start()

    eye = lane == row
    live = lane < hd
    live1 = live[0:1, :]

    def owner_a(b):
        tau = tau_v[me]
        with scope("wait_g"):
            all_of(g_recv.at[b], g_ssem, g_rsem.at[b]).wait_recv()
        total = g_send[b, me]
        for off in range(1, n):
            total = total + g_recv[b, off - 1]
        gram = unpack(total[0:half, :])
        sums = jnp.zeros((8, LANES), F32)
        for i in range(3):
            mine = (lane[0:8, :] >= 16 * i) & (lane[0:8, :] < 16 * i + 16)
            sums = jnp.where(mine, roll(total[8 * i:8 * i + 8, :], 16 * i - hd), sums)
        ssq = sums[0:1, :]
        ssk = sums[1:2, :]
        rq_col = jnp.sum(jnp.where(eye, lax.rsqrt(ssq), 0.0), axis=1, keepdims=True)
        scale = jnp.where(live, tau * rq_col * lax.rsqrt(ssk), 0.0)
        logits = jnp.where(live, gram * scale, 0.0)
        top = jnp.max(jnp.where(live, logits, -jnp.inf), axis=1, keepdims=True)
        e = jnp.where(live, jnp.exp(logits - top), 0.0)
        p = e / jnp.sum(e, axis=1, keepdims=True)
        back_a[b, me] = pack(p, 0).astype(BF16)
        for off in range(1, n):
            a_copy(b, off).start()
        return p, logits, scale, ssq, ssk

    def owner_g(b, state):
        p, logits, scale, ssq, ssk = state
        with scope("wait_p"):
            all_of(p_recv.at[b], p_ssem, p_rsem.at[b]).wait_recv()
        total = p_send[b, me]
        for off in range(1, n):
            total = total + p_recv[b, off - 1]
        dprob = jnp.where(live, unpack(total), 0.0).astype(BF16).astype(F32)
        glog = p * (dprob - jnp.sum(p * dprob, axis=1, keepdims=True))
        weighted = glog * logits
        w_row = jnp.sum(weighted, axis=1, keepdims=True)
        cq = -jnp.sum(jnp.where(eye, w_row, 0.0), axis=0, keepdims=True)
        cq = jnp.where(live1, cq / ssq, 0.0)
        ck = jnp.where(live1, -jnp.sum(weighted, axis=0, keepdims=True) / ssk, 0.0)
        c_rows = jnp.concatenate([cq, ck, jnp.zeros((6, LANES), F32)], axis=0)
        back_g[b, me] = (pack(glog * scale, 0) + beside(c_rows, 0)).astype(BF16)
        for off in range(1, n):
            d_copy(b, off).start()
        return jnp.sum(w_row, axis=0, keepdims=True)

    def build(b, got_of, ssem, rsem, bd, name):
        with scope(name):
            all_of(got_of.at[b, pl.ds(0, n - 1)], ssem, rsem.at[b]).wait_recv()
        found_rows = [jnp.zeros((8, LANES), F32) for _ in range(tiles)]
        for h in range(heads):
            got = got_of[b, h].astype(F32)
            which, first, found = pieces(h)
            s = first % LANES
            val = jnp.concatenate([roll(got, s), roll(got, s + 64)], axis=0)
            cols = [jnp.zeros((hd, LANES), F32) for _ in range(2)]
            for t, lo, hi in found:
                cols[t] = jnp.where((lane >= lo) & (lane < hi), val, 0.0)
            bd[b, which, first:first + hd, :] = jnp.concatenate(cols, axis=1).astype(BF16)
            for i in range(3):
                t, lo = divmod(h * hd + 16 * i, LANES)
                mine = (lane[0:8, :] >= lo) & (lane[0:8, :] < lo + 16)
                found_rows[t] = jnp.where(mine, roll(got[8 * i:8 * i + 8, :], lo - hd), found_rows[t])
        return found_rows

    def clear(bd):
        for b in range(images):
            bd[b, 0, SPLIT * hd:256, :] = jnp.zeros((256 - SPLIT * hd, 256), BF16)
            bd[b, 1, 0:SPLIT * hd - LANES, :] = jnp.zeros((SPLIT * hd - LANES, 256), BF16)

    def build_a(b):
        build(b, back_a, a_ssem, a_rsem, bd_a, "wait_a")

    def build_g(b):
        c_v[b] = jnp.concatenate(build(b, back_g, d_ssem, d_rsem, bd_g, "wait_d"), axis=1)

    def per_head(tok, mats, transposed):
        c = 1 if transposed else 0
        left = dot(tok[:, 0:256], mats[0], 1, c)
        right = dot(tok[:, 128:384], mats[1], 1, c)
        return jnp.concatenate([left[:, 0:128], left[:, 128:256] + right[:, 0:128], right[:, 128:256]], axis=1)

    def cols(c):
        return pl.ds(STARTS[c], STARTS[c + 1] - STARTS[c])

    def pair_copy(c):
        return pltpu.make_async_remote_copy(
            src_ref=part.at[:, :, 1 - core, :, :, cols(c)], dst_ref=pair_recv.at[:, :, :, :, cols(c)],
            send_sem=pair_ssem, recv_sem=pair_rsem.at[c],
            device_id=dev(partner), device_id_type=MESH)

    def arrival_sem(c, stage):
        if stage == FAR:
            return far_rsem.at[c]
        return near_rsem if stage == NEAR else passed_rsem.at[0 if c < LATE else 1]

    def stage_copies(c, stage):
        if stage == FAR:
            refs = ((chip_sum.at[1 - py, 1 - px, 0, :, cols(c)], x_recv.at[1 - py, :, cols(c)], dev_x),
                    (chip_sum.at[1 - py, 1 - px, 1, :, cols(c)], y_recv.at[1 - px, :, cols(c)], dev_y))
        elif stage == NEAR:
            refs = ((chip_sum.at[py, 1 - px, 0, :, cols(c)], x_recv.at[py, :, cols(c)], dev_x),
                    (chip_sum.at[1 - py, px, 1, :, cols(c)], y_recv.at[px, :, cols(c)], dev_y))
        else:
            refs = ((x_send2.at[:, cols(c)], x_recv2.at[:, cols(c)], dev_x),
                    (y_send2.at[:, cols(c)], y_recv2.at[:, cols(c)], dev_y))
        return [pltpu.make_async_remote_copy(
            src_ref=src, dst_ref=dst, send_sem=st_ssem.at[stage], recv_sem=arrival_sem(c, stage),
            device_id=dev(d), device_id_type=MESH) for src, dst, d in refs]

    def weight_part(b, col, lhs, rhs, contract):
        value = dot(lhs, rhs, contract, 0).reshape(2, 2, 2, 2, half, dim)
        if b:
            value = value + part[:, :, :, :, :, col:col + dim]
        part[:, :, :, :, :, col:col + dim] = value

    def part_o(b):
        weight_part(b, 0, o_v[rows(b), :], dy_v[rows(b), :], 0)

    def part_qkv(b, i):
        weight_part(b, (1 + i) * dim, ut_v[:, b * tokens:(b + 1) * tokens], dqkv_v[rows(b), i * dim:(i + 1) * dim], 1)

    def rs0(c):
        pair_copy(c).start()

    def rs1(*chunks):
        for c in chunks:
            with scope("wait_pair"):
                pair_copy(c).wait_recv()
            chip_sum[:, :, :, :, cols(c)] = part[:, :, core, :, :, cols(c)] + pair_recv[:, :, :, :, cols(c)]
            for copy in stage_copies(c, FAR):
                copy.start()
        for c in chunks:
            for copy in stage_copies(c, NEAR):
                copy.start()

    def rs2(c):
        with scope("wait_st0"):
            all_of(x_recv.at[:, :, cols(c)], st_ssem.at[FAR], far_rsem.at[c]).wait_recv()
        x_send2[:, cols(c)] = chip_sum[py, 1 - px, 1, :, cols(c)] + y_recv[1 - px, :, cols(c)]
        y_send2[:, cols(c)] = chip_sum[1 - py, px, 0, :, cols(c)] + x_recv[1 - py, :, cols(c)]
        for copy in stage_copies(c, PASSED):
            copy.start()

    def rs3(lo, hi):
        own_a = chip_sum[py, px, 0, :, lo:hi] + x_recv[py, :, lo:hi]
        own_b = chip_sum[py, px, 1, :, lo:hi] + y_recv[px, :, lo:hi]
        return jnp.concatenate([own_a + y_recv2[:, lo:hi], own_b + x_recv2[:, lo:hi]], axis=0).astype(BF16)

    def heads_out(b):
        rs = rows(b)
        o_v[rs, :] = per_head(qkv_v[rs, 0:dim], bd_a[b], True).astype(BF16)

    def grad_v(b):
        rs = rows(b)
        dqkv_v[rs, 0:dim] = per_head(do_v[rs, :], bd_a[b], False).astype(BF16)

    def grad_q(b):
        rs = rows(b)
        q = qkv_v[rs, dim:2 * dim]
        k = qkv_v[rs, 2 * dim:3 * dim]
        dqkv_v[rs, dim:2 * dim] = (per_head(k, bd_g[b], True) + c_v[b, 0:1, :] * q.astype(F32)).astype(BF16)

    def grad_k(b):
        rs = rows(b)
        q = qkv_v[rs, dim:2 * dim]
        k = qkv_v[rs, 2 * dim:3 * dim]
        dqkv_v[rs, 2 * dim:3 * dim] = (per_head(q, bd_g[b], False) + c_v[b, 1:2, :] * k.astype(F32)).astype(BF16)

    def out_y(b):
        rs = rows(b)
        y_v[rs, :] = (x_v[rs, :].astype(F32) + dot(o_v[rs, :], wout_v[...], 1, 0)).astype(BF16)

    def grad_u(b, i):
        rs = pl.ds(b * tokens + i * (tokens // 2), tokens // 2)
        du = dot(dqkv_v[rs, :], wqkv_v[...], 1, 1).astype(BF16)
        du_v[rs, :] = du
        du = du.astype(F32)
        return jnp.sum(du * xhat_v[rs, :], axis=0, keepdims=True), jnp.sum(du, axis=0, keepdims=True)

    def out_dx(b):
        rs = rows(b)
        gain = gain_v[...].reshape(1, dim)
        xhat = xhat_v[rs, :]
        a = du_v[rs, :].astype(F32) * gain
        ma = jnp.mean(a, axis=-1, keepdims=True)
        mx = jnp.mean(a * xhat, axis=-1, keepdims=True)
        dx_v[rs, :] = (dy_v[rs, :].astype(F32) + rstd_v[rs, :] * (a - ma - xhat * mx)).astype(BF16)

    with scope("phase_1"):
        clear(bd_a)
        clear(bd_g)
        load_x(0).wait()
        load_gain.wait()
        load_bias.wait()
        layer_norm(0)
        load_qk.wait()
        load_x(1).wait()
        project_qk(0)
        layer_norm(1)
        gram_part(0)
    with scope("wait_barrier"):
        pl.semaphore_wait(barrier, n - 1)
    with scope("phase_2"):
        send_g(0)
        project_qk(1)
        gram_part(1)
        send_g(1)
    with scope("phase_3"):
        load_wout.wait()
        pltpu.make_async_copy(dy_v, dy_v, load_sem.at[images]).wait()
        load_v.wait()
        load_tau.wait()
        project_v(0)
        grad_o(0)
        prob_part(0)
        send_p(0)
        grad_o(1)
        project_v(1)
    with scope("owner_a0"):
        state0 = owner_a(0)
    with scope("phase_4"):
        prob_part(1)
        send_p(1)
    with scope("owner_a1"):
        state1 = owner_a(1)
    with scope("transpose"):
        for b in range(images):
            ut_v[:, b * tokens:(b + 1) * tokens] = u_v[rows(b), :].T
    with scope("owner_g0"):
        w0 = owner_g(0, state0)
    build_a(0)
    with scope("group1"):
        heads_out(0)
        grad_v(0)
        part_o(0)
    with scope("owner_g1"):
        w1 = owner_g(1, state1)
    build_a(1)
    with scope("group2"):
        heads_out(1)
        part_o(1)
        rs0(0)
    with scope("group3"):
        part_qkv(0, 0)
        grad_v(1)
        part_qkv(1, 0)
        rs0(1)
    rs1(0)
    build_g(0)
    with scope("group4"):
        grad_q(0)
        part_qkv(0, 1)
        grad_k(0)
    build_g(1)
    with scope("group4b"):
        grad_q(1)
    rs1(1)
    with scope("group5"):
        part_qkv(1, 1)
        rs0(2)
        grad_k(1)
        part_qkv(0, 2)
    rs2(0)
    with scope("group6"):
        part_qkv(1, 2)
        rs0(3)
        rs0(4)
    rs1(2)
    ln_sums = []
    with scope("group7"):
        out_y(0)
        out_y(1)
    rs1(3, 4)
    rs2(1)
    with scope("group8"):
        ln_sums.append(grad_u(0, 0))
        ln_sums.append(grad_u(0, 1))
        ln_sums.append(grad_u(1, 0))
    rs2(2)
    with scope("group8b"):
        ln_sums.append(grad_u(1, 1))

    sg = sum(val[0] for val in ln_sums)
    sb = sum(val[1] for val in ln_sums)
    st = jnp.where(lane[0:1, :] == me, (w0 + w1) / tau_v[me], 0.0)
    ln_rows = [val[:, t * LANES:(t + 1) * LANES] for val in (sg, sb) for t in range(tiles)]
    ln_all[me] = jnp.concatenate(ln_rows + [st, jnp.zeros((1, LANES), F32)], axis=0)

    def ln_copy(off):
        return pltpu.make_async_remote_copy(
            src_ref=ln_all.at[me], dst_ref=ln_all.at[me], send_sem=ln_ssem, recv_sem=ln_rsem,
            device_id=dev(peers[off - 1]), device_id_type=MESH)

    for off in range(1, n):
        ln_copy(off).start()

    rs2(3)
    rs2(4)
    with scope("group9"):
        out_dx(0)
        out_dx(1)
    split = STARTS[LATE]
    with scope("wait_near"):
        all_of(x_recv, st_ssem.at[NEAR], near_rsem).wait_recv()
    with scope("wait_st1"):
        all_of(x_recv.at[:, :, pl.ds(0, split)], st_ssem.at[PASSED], passed_rsem.at[0]).wait_recv()
    gwout_ref[...] = rs3(0, dim)
    gwqkv_ref[:, 2 * dim:3 * dim] = rs3(dim, 2 * dim)
    gwqkv_ref[:, 0:dim] = rs3(2 * dim, 3 * dim)
    with scope("wait_ln"):
        all_of(ln_all.at[pl.ds(0, n - 1)], ln_ssem, ln_rsem).wait_recv()
    sums = ln_all[0]
    for d in range(1, n):
        sums = sums + ln_all[d]
    sums_ref[...] = sums
    with scope("wait_st1"):
        all_of(x_recv.at[:, :, pl.ds(split, 4 * dim - split)], st_ssem.at[PASSED], passed_rsem.at[1]).wait_recv()
    gwqkv_ref[:, dim:2 * dim] = rs3(3 * dim, 4 * dim)

    with scope("final"):
        all_of(g_recv, g_ssem, g_rsem.at[0]).wait_send()
        all_of(p_recv, p_ssem, p_rsem.at[0]).wait_send()
        all_of(back_a.at[:, pl.ds(0, n - 1)], a_ssem, a_rsem.at[0]).wait_send()
        all_of(back_g.at[:, pl.ds(0, n - 1)], d_ssem, d_rsem.at[0]).wait_send()
        all_of(pair_recv, pair_ssem, pair_rsem.at[0]).wait_send()
        for stage in (FAR, NEAR, PASSED):
            all_of(x_recv, st_ssem.at[stage], near_rsem).wait_send()
        all_of(ln_all.at[pl.ds(0, n - 1)], ln_ssem, ln_rsem).wait_send()


def finish(dim, heads, y_v, dx_v, gwqkv_v, gwout_v, sums_v,
           y_hbm, dx_hbm, gwqkv_hbm, gwout_hbm, ggain_hbm, gbias_hbm, gtau_hbm,
           gain_v, bias_v, tau_v, sem):
    tiles = dim // LANES
    pairs = ((y_v, y_hbm), (dx_v, dx_hbm), (gwqkv_v, gwqkv_hbm), (gwout_v, gwout_hbm),
             (gain_v, ggain_hbm), (bias_v, gbias_hbm), (tau_v, gtau_hbm))
    copies = [pltpu.make_async_copy(src, dst, sem.at[i]) for i, (src, dst) in enumerate(pairs)]
    for copy in copies[:4]:
        copy.start()
    for t in range(tiles):
        gain_v[t * LANES:(t + 1) * LANES] = sums_v[t, :]
        bias_v[t * LANES:(t + 1) * LANES] = sums_v[tiles + t, :]
    tau_v[...] = sums_v[2 * tiles, 0:heads]
    for copy in copies[4:]:
        copy.start()
    for copy in copies:
        copy.wait()


def solution(mesh):
    n = mesh.shape["sp"]

    def local_step(x_in, grad_y, ln_gain, ln_bias, w_qkv, w_out, temp_tau):
        images, tokens, dim = x_in.shape
        heads = temp_tau.shape[0]
        hd = dim // heads
        half = hd // 2
        num = images * tokens
        hbm = pl.BlockSpec(memory_space=pltpu.HBM)
        vmem = pl.BlockSpec(memory_space=pltpu.VMEM)
        dma = pltpu.SemaphoreType.DMA
        params = pltpu.CompilerParams(collective_id=0, has_side_effects=True, vmem_limit_bytes=KERNEL_VMEM)
        y, dx, gwqkv, gwout, sums = pl.pallas_call(
            functools.partial(body, images, tokens, dim, heads, n),
            out_shape=(
                pltpu.VMEM((num, dim), BF16),
                pltpu.VMEM((num, dim), BF16),
                pltpu.VMEM((hd, 3 * dim), BF16),
                pltpu.VMEM((hd, dim), BF16),
                pltpu.VMEM((8, LANES), F32),
            ),
            in_specs=[hbm] * 7,
            out_specs=(vmem, vmem, vmem, vmem, vmem),
            scratch_shapes=[
                pltpu.VMEM((num, dim), BF16),
                pltpu.VMEM((num, dim), BF16),
                pltpu.VMEM((dim,), F32),
                pltpu.VMEM((dim,), F32),
                pltpu.SMEM((heads,), F32),
                pltpu.VMEM((dim, 3 * dim), BF16),
                pltpu.VMEM((dim, dim), BF16),
                pltpu.VMEM((num, dim), F32),
                pltpu.VMEM((num, 1), F32),
                pltpu.VMEM((num, dim), BF16),
                pltpu.VMEM((num, dim), BF16),
                pltpu.VMEM((dim, num), BF16),
                pltpu.VMEM((num, 3 * dim), BF16),
                pltpu.VMEM((num, dim), BF16),
                pltpu.VMEM((num, dim), BF16),
                pltpu.VMEM((num, 3 * dim), BF16),
                pltpu.VMEM((images, heads, G_ROWS, LANES), F32),
                pltpu.VMEM((images, n - 1, G_ROWS, LANES), F32),
                pltpu.VMEM((images, heads, P_ROWS, LANES), F32),
                pltpu.VMEM((images, n - 1, P_ROWS, LANES), F32),
                pltpu.VMEM((images, heads, BACK_ROWS, LANES), BF16),
                pltpu.VMEM((images, heads, BACK_ROWS, LANES), BF16),
                pltpu.VMEM((images, 2, 256, 256), BF16),
                pltpu.VMEM((images, 2, 256, 256), BF16),
                pltpu.VMEM((images, 8, dim), F32),
                pltpu.VMEM((2, 2, 2, 2, half, 4 * dim), F32),
                pltpu.VMEM((2, 2, 2, half, 4 * dim), F32),
                pltpu.VMEM((2, 2, 2, half, 4 * dim), F32),
                pltpu.VMEM((2, half, 4 * dim), F32),
                pltpu.VMEM((2, half, 4 * dim), F32),
                pltpu.VMEM((half, 4 * dim), F32),
                pltpu.VMEM((half, 4 * dim), F32),
                pltpu.VMEM((half, 4 * dim), F32),
                pltpu.VMEM((half, 4 * dim), F32),
                pltpu.VMEM((n, 8, LANES), F32),
                dma((images + 7,)),
                dma, dma((images,)),
                dma, dma((images,)),
                dma, dma((images,)),
                dma, dma((images,)),
                dma, dma((5,)),
                dma((3,)), dma((5,)), dma, dma((2,)),
                dma, dma,
            ],
            compiler_params=params,
            name="xca_step",
        )(x_in, grad_y, ln_gain, ln_bias, w_qkv, w_out, temp_tau)
        y, dx, gwqkv, gwout, ggain, gbias, gtau = pl.pallas_call(
            functools.partial(finish, dim, heads),
            out_shape=(
                jax.ShapeDtypeStruct((num, dim), BF16),
                jax.ShapeDtypeStruct((num, dim), BF16),
                jax.ShapeDtypeStruct((hd, 3 * dim), BF16),
                jax.ShapeDtypeStruct((hd, dim), BF16),
                jax.ShapeDtypeStruct((dim,), F32),
                jax.ShapeDtypeStruct((dim,), F32),
                jax.ShapeDtypeStruct((heads,), F32),
            ),
            in_specs=[vmem] * 5,
            out_specs=(hbm,) * 7,
            scratch_shapes=[pltpu.VMEM((dim,), F32), pltpu.VMEM((dim,), F32), pltpu.VMEM((heads,), F32), dma((7,))],
            compiler_params=pltpu.CompilerParams(vmem_limit_bytes=2**20),
            name="xca_finish",
        )(y, dx, gwqkv, gwout, sums)
        return y.reshape(x_in.shape), dx.reshape(x_in.shape), gwqkv, gwout, ggain, gbias, gtau

    token_spec = P("dp", "sp", None)
    return jax.shard_map(local_step, mesh=mesh, in_specs=(token_spec, token_spec, P(), P(), P(), P(), P()), out_specs=(token_spec, token_spec, P(("dp", "sp"), None), P(("dp", "sp"), None), P("dp"), P("dp"), P("dp")), check_vma=False)
```
